32 devices in a mesh: parts: 2 (over y), sub: 4 (over z), row: 2 (over x), col: 2 (over core).
Axes of the slice: x: 2, y: 2, z: 4, core: 2. Of those that a mesh axis runs over, the one named last changes fastest.
Arguments:
- loads: float32 [8, 32, 1024], P(('parts', 'sub'), 'col'), parts along dimension 0, may hold values from -6 to 6
- weights: float32 [8, 1024], P(('parts', 'sub')), parts along dimension 0, may hold values from 0.25 to 4
- dual_ops: bfloat16 [8, 2048, 2048], P(('parts', 'sub'), 'row'), parts along dimension 0, as said below
- corner_maps: bfloat16 [8, 24, 2048], P(('parts', 'sub'), None, 'row'), parts along dimension 0, may hold values from -0.25 to 0.25
- coarse_inverse: float32 [96, 48], P('parts'), parts along dimension 0, as said below
- corner_ids: int32 [8, 24], P('parts'), parts along dimension 0, may hold values from 0 to 47, as said below
- iface_sizes: int32 [8], P('parts'), parts along dimension 0, may hold values from 512 to 1024, as said below
- left_partner: int32 [8, 1024], P(('parts', 'sub')), parts along dimension 0, may hold values from 0 to 1023, as said below
- right_partner: int32 [8, 1024], P(('parts', 'sub')), parts along dimension 0, may hold values from 0 to 1023, as said below
Outputs:
- solution: float32 [8, 32, 1024], P(('parts', 'sub'), 'col'), parts along dimension 0
- residual: float32 [8, 32, 1024], P(('parts', 'sub'), 'col'), parts along dimension 0
The draws below stay inside these ranges and needn't reach their ends.
There are 2 independent parts, one for each index of `parts`. The reference program is written for one: setup_inputs(seed, part) draws one part's arguments, and reference() takes and returns one part's arrays. A program takes and returns all parts, laid end to end along the dimension named above; each array names one. Nothing has to cross between parts.
Inputs may be any that keep to these rules, and one draw needn't show every extreme that they name: Global indices 24/2 * s to 24/2 * s + 24/2 - 1 are the corners of the interface between s and s+1; the first half of subdomain s's corner_ids is a permutation of those of interface s-1, the second half a permutation of those of interface s. `left_partner`: each row s is a permutation that maps the slots below iface_sizes[s-1] onto slots below it. `right_partner`: each row s is a permutation that maps the slots below iface_sizes[s] onto slots below it, and is the inverse of left_partner[s+1]. `dual_ops`: symmetric positive definite. `coarse_inverse`: symmetric positive definite. For each s < 2, one of iface_sizes[s] and iface_sizes[s + 2] is 896 or more and the other 640 or less.
All inputs are finite; a program needn't handle non-finite values.
Results may differ from the reference program's by a relative error of at most 0.015.
Values may be sent and summed in bfloat16 or wider, within the bound.
A program may use at most 64 MiB of HBM per device.

```python
import math
import jax
import jax.numpy as jnp
from jax import lax

ORDER = 2048
COLS = 32
C_LOC = 24
ITERS = 2
S = 4
HALF = 1024
NC = 48


def draw_dual_ops(key, part):

    def one_matrix(sub_key):
        first, second = jax.random.split(sub_key)
        noise = jax.random.normal(first, (ORDER, ORDER), jnp.float32)
        spread = 0.35
        diagonal = jax.random.uniform(second, (ORDER,), jnp.float32, 1.0, 3.0)
        symmetric = (noise + noise.T) * (spread / (2.0 * ORDER) ** 0.5)
        return (symmetric + jnp.diag(diagonal)).astype(jnp.bfloat16)
    return lax.map(one_matrix, jax.random.split(key, S))


def draw_coarse_inverse(key, part):
    first, second = jax.random.split(jax.random.fold_in(key, 3))
    noise = jax.random.normal(first, (NC, NC), jnp.float32)
    spread = 0.5
    diagonal = jax.random.uniform(second, (NC,), jnp.float32, 1.5, 3.0)
    symmetric = (noise + noise.T) * (spread / (2.0 * NC) ** 0.5)
    return symmetric + jnp.diag(diagonal)


def draw_corner_ids(key, part):
    width = C_LOC // 2
    keys = jax.random.split(jax.random.fold_in(key, 5), 2 * S)
    orders = jax.vmap(lambda one_key: jax.random.permutation(one_key, width))(keys).astype(jnp.int32)
    subdomains = jnp.arange(S, dtype=jnp.int32)
    before = width * ((subdomains + S - 1) % S)[:, None] + orders[:S]
    after = width * subdomains[:, None] + orders[S:]
    return jnp.concatenate([before, after], axis=1).astype(jnp.int32)


def interface_sizes(key):
    first, second, third = jax.random.split(jax.random.fold_in(key, 11), 3)
    pairs = S // 2
    light = jax.random.randint(first, (pairs,), HALF // 2, 5 * HALF // 8 + 1, dtype=jnp.int32)
    heavy = jax.random.randint(second, (pairs,), 7 * HALF // 8, HALF + 1, dtype=jnp.int32)
    flip = jax.random.randint(third, (pairs,), 0, 2, dtype=jnp.int32)
    lower = jnp.where(flip == 1, heavy, light)
    upper = jnp.where(flip == 1, light, heavy)
    return jnp.concatenate([lower, upper]).astype(jnp.int32)


def draw_iface_sizes(key, part):
    return interface_sizes(key)


def interface_orders(key):
    sizes = interface_sizes(key)
    keys = jax.random.split(jax.random.fold_in(key, 7), S)
    slots = jnp.arange(HALF, dtype=jnp.int32)

    def one_order(one_key, count):
        ranks = jax.random.permutation(one_key, HALF).astype(jnp.int32)
        scores = ranks + HALF * (slots >= count).astype(jnp.int32)
        return jnp.argsort(scores, stable=True).astype(jnp.int32)
    return jax.vmap(one_order)(keys, sizes).astype(jnp.int32)


def draw_left_partner(key, part):
    return jnp.roll(interface_orders(key), 1, axis=0).astype(jnp.int32)


def draw_right_partner(key, part):
    return jnp.argsort(interface_orders(key), axis=1, stable=True).astype(jnp.int32)


def block_scale(key, extent, shards, least, largest):
    level, own = 1.0, jax.random.fold_in(key, 6)
    for dim, blocks in shards:
        steps = jnp.exp(jax.random.uniform(jax.random.fold_in(own, dim), (blocks,), jnp.float32, least / len(shards), largest / len(shards)))
        level = level * jnp.repeat(steps, extent[dim] // blocks).reshape([-1 if axis == dim else 1 for axis in range(len(extent))])
    return level


def centred(stream_key, dims, scale, reach, cuts=(), kind=jnp.bfloat16):
    level = block_scale(stream_key, dims, cuts, -0.22, 0.18) if cuts else 1.0
    entries = jax.random.normal(stream_key, dims, jnp.float32) * scale * level
    return jnp.minimum(jnp.maximum(entries, -reach), reach).astype(kind)


def setup_inputs(seed: int = 0, part: int = 0) -> dict:
    key_of = jax.random.split(jax.random.key(seed), 10)
    part_keys = jax.random.split(jax.random.fold_in(key_of[9], part), 10)
    return {
        "loads": centred(part_keys[0], (S, COLS, HALF), 1.0, 6.0, ((0, 4), (1, 2)), jnp.float32),
        "weights": jnp.clip(jnp.exp(math.log(4.0) - 2.7725887 * jax.random.uniform(part_keys[1], (S, HALF), jnp.float32) ** block_scale(part_keys[1], (S, HALF), ((0, 4),), -0.2, 0.2)), 0.25, 4.0),
        "dual_ops": draw_dual_ops(jax.random.fold_in(jax.random.fold_in(key_of[9], part), 71), part),
        "corner_maps": centred(part_keys[3], (S, C_LOC, ORDER), (ORDER // 4) ** -0.5, 0.25, ((0, 4), (2, 2))),
        "coarse_inverse": draw_coarse_inverse(jax.random.fold_in(jax.random.fold_in(key_of[9], part), 71), part),
        "corner_ids": draw_corner_ids(jax.random.fold_in(jax.random.fold_in(key_of[9], part), 71), part),
        "iface_sizes": draw_iface_sizes(jax.random.fold_in(jax.random.fold_in(key_of[9], part), 71), part),
        "left_partner": draw_left_partner(jax.random.fold_in(jax.random.fold_in(key_of[9], part), 71), part),
        "right_partner": draw_right_partner(jax.random.fold_in(jax.random.fold_in(key_of[9], part), 71), part),
    }


def apply_operator(vec, dual_ops, corner_maps, coarse_inverse, corner_ids, left_partner, right_partner, live):
    ahead = jnp.roll(vec, -1, axis=0)
    right_index = jnp.broadcast_to(right_partner[:, None, :], vec.shape)
    right_side = jnp.take_along_axis(ahead, right_index, axis=2)
    full = jnp.concatenate([vec, right_side], axis=2).astype(jnp.bfloat16)

    def one_local(items):
        piece, matrix, coupling = items
        local = jnp.dot(piece, matrix, preferred_element_type=jnp.float32)
        corner = jnp.dot(piece, coupling.T, preferred_element_type=jnp.float32)
        return local, corner

    local, corner = lax.map(one_local, (full, dual_ops, corner_maps))
    columns = jnp.arange(NC, dtype=jnp.int32)
    onehot = (corner_ids[:, :, None] == columns[None, None, :]).astype(jnp.float32)
    coarse = jnp.einsum("scj,sjn->cn", corner, onehot, precision=lax.Precision.HIGHEST)
    solved = jnp.dot(coarse, coarse_inverse, precision=lax.Precision.HIGHEST)
    back = jnp.einsum("cn,sjn->scj", solved, onehot, precision=lax.Precision.HIGHEST).astype(jnp.bfloat16)

    def one_back(items):
        piece, coupling = items
        return jnp.dot(piece, coupling, preferred_element_type=jnp.float32)

    united = local + lax.map(one_back, (back, corner_maps))
    upper = jnp.roll(united[:, :, HALF:], 1, axis=0)
    left_index = jnp.broadcast_to(left_partner[:, None, :], vec.shape)
    return (united[:, :, :HALF] + jnp.take_along_axis(upper, left_index, axis=2)) * live[:, None, :]


def reference(loads, weights, dual_ops, corner_maps, coarse_inverse, corner_ids, iface_sizes, left_partner, right_partner):
    slots = jnp.arange(HALF, dtype=jnp.int32)
    live = (slots[None, :] < jnp.roll(iface_sizes, 1)[:, None]).astype(jnp.float32)
    scaling = weights[:, None, :]
    residual = loads * live[:, None, :]
    solution = jnp.zeros_like(residual)
    precond = scaling * residual
    direction = precond
    rz_value = jnp.sum(residual * precond, axis=(0, 2))
    for step in range(ITERS):
        image = apply_operator(direction, dual_ops, corner_maps, coarse_inverse, corner_ids, left_partner, right_partner, live)
        alpha = rz_value / jnp.sum(direction * image, axis=(0, 2))
        solution = solution + alpha[None, :, None] * direction
        residual = residual - alpha[None, :, None] * image
        precond = scaling * residual
        new_value = jnp.sum(residual * precond, axis=(0, 2))
        direction = precond + (new_value / rz_value)[None, :, None] * direction
        rz_value = new_value
    return solution, residual
```

```python
import functools

import jax
import jax.numpy as jnp
from jax import lax
from jax.experimental import pallas as pl
from jax.experimental.pallas import tpu as pltpu
from jax.sharding import PartitionSpec as P

MESH = pl.DeviceIdType.MESH
LIMIT = 40 * 2**20
BF = jnp.bfloat16
F32 = jnp.float32


def each(count, body):
    if count <= 8:
        for at in range(count):
            body(at)
    else:
        lax.fori_loop(0, count, lambda at, _: (body(at), 0)[1], 0)


def dot_nt(a, b):
    return lax.dot_general(a, b, (((1,), (1,)), ((), ())), preferred_element_type=F32)


def dot_nn(a, b):
    return lax.dot_general(a, b, (((1,), (0,)), ((), ())), preferred_element_type=F32)


def kernel(
    S, R, loads, weights, op, cm, cinv, ids, sizes, lmap, rmap, sol, res,
    loads_v, w_v, op_v, cv, cinv_p, ids_v, lmap_v, rmap_v, sizes_v,
    zsend, zrecv, wrecv, cmo, cmn, mo, mn, pl_m, pr_m, zs, acc,
    own, nbr, pk, dk,
    in_sem, op_sem, z_sem, cmo_ssem, cmo_rsem, cmn_ssem, cmn_rsem,
    own_ssem, own_rsem, nbr_ssem, nbr_rsem, pk_ssem, pk_rsem, dk_ssem, dk_rsem,
):
    s = lax.axis_index("sub")
    r = lax.axis_index("row")
    G = S * R
    me = s * R + r
    C, H = loads_v.shape
    B = op_v.shape[0]
    NC = cv.shape[0]
    W = cinv_p.shape[0]
    half_r = R // 2
    nxt = lax.rem(s + 1, S)
    prv = lax.rem(s + S - 1, S)
    side = r // half_r
    toward = lax.rem(s + S - 1 + 2 * side, S)

    barrier = pltpu.get_barrier_semaphore()

    def peer(k):
        g = lax.rem(me + k + 1, G)
        return g, {"sub": g // R, "row": lax.rem(g, R)}

    def greet(k):
        _, who = peer(k)
        pl.semaphore_signal(barrier, inc=1, device_id=who, device_id_type=MESH)

    each(G - 1, greet)

    ins = [
        pltpu.make_async_copy(src, dst, in_sem.at[i])
        for i, (src, dst) in enumerate([
            (loads.at[0], loads_v), (weights, w_v), (sizes, sizes_v), (rmap, rmap_v), (lmap, lmap_v),
            (ids, ids_v), (cinv, cv), (cm.at[0], cmo.at[r]),
        ])
    ]
    for copy in ins:
        copy.start()
    op_copy = pltpu.make_async_copy(op.at[0], op_v, op_sem)
    op_copy.start()

    for copy in ins[:3]:
        copy.wait()
    lanes = lax.broadcasted_iota(jnp.int32, (1, H), 1)
    live_l = (lanes < sizes_v[prv]).astype(F32)
    size_after = sizes_v[s]
    w_l = w_v[...]
    r0 = loads_v[...] * live_l
    z0 = w_l * r0
    zsend[...] = z0.astype(BF)

    pl.semaphore_wait(barrier, G - 1)

    def remote(src, dst, ssem, rsem, who):
        return pltpu.make_async_remote_copy(
            src_ref=src, dst_ref=dst, send_sem=ssem, recv_sem=rsem, device_id=who, device_id_type=MESH
        )

    z_copy = remote(zsend, zrecv, z_sem.at[0], z_sem.at[1], {"sub": prv})
    w_copy = remote(w_v, wrecv, z_sem.at[2], z_sem.at[3], {"sub": prv})
    z_copy.start()
    w_copy.start()

    def to_row(src, dst, ssem, rsem, k):
        q = lax.rem(r + k, R)
        return remote(src, dst.at[r], ssem.at[k], rsem.at[r], {"row": q})

    def to_side(src, dst, ssem, rsem, k):
        q = lax.rem(r + k, R)
        return remote(src, dst.at[r], ssem.at[k], rsem.at[r], {"sub": toward, "row": q})

    def wait_slot(dst, ssem, rsem, q):
        remote(dst.at[q], dst.at[q], ssem.at[0], rsem.at[q], {"sub": nxt}).wait_recv()

    cm_sends = [to_side(cm.at[0], cmn, cmn_ssem, cmn_rsem, k) for k in range(R)]
    cm_sends += [to_row(cm.at[0], cmo, cmo_ssem, cmo_rsem, k) for k in range(1, R)]

    def send_maps():
        for copy in cm_sends:
            copy.start()

    ins[3].wait()
    ins[4].wait()
    right_map = rmap_v[...]
    left_map = lmap_v[...]
    live_r = (right_map < size_after).astype(F32)

    def hot(target, the_map):
        step = 128
        for c in range(H // step):
            rows = lax.broadcasted_iota(jnp.int32, (step, H), 0) + c * step
            target[pl.ds(c * step, step), :] = (rows == the_map).astype(F32).astype(BF)

    hot(pr_m, right_map)
    hot(pl_m, left_map)
    ins[5].wait()
    ins[6].wait()
    cinv_p[...] = jnp.zeros_like(cinv_p)
    cinv_p[0:NC, 0:NC] = cv[...]

    def hot_ids(t):
        row = ids_v[pl.ds(t, 1), :]
        rows = lax.broadcasted_iota(jnp.int32, (W, row.shape[1]), 0)
        return (rows == row).astype(F32).astype(BF)

    hot_own = hot_ids(s)
    ins[7].wait()
    mo[r] = dot_nn(hot_own, cmo[r]).astype(BF)

    pl.when(s == S - 1)(send_maps)

    op_copy.wait()
    acc[...] = dot_nt(z0.astype(BF), op_v[:, :H])

    z_copy.wait_recv()
    w_copy.wait_recv()
    w_in = wrecv[...]
    w_hi = w_in.astype(BF)
    w_lo = (w_in - w_hi.astype(F32)).astype(BF)
    pad = lax.broadcasted_iota(jnp.int32, (16, H), 0)
    w_rows = jnp.where(pad == 0, w_hi.astype(F32), jnp.where(pad == 1, w_lo.astype(F32), 0.0))
    gathered = dot_nn(jnp.concatenate([zrecv[...], w_rows.astype(BF)], axis=0), pr_m[...])
    z0_r = gathered[:C]
    w_r = gathered[C : C + 1] + gathered[C + 1 : C + 2]

    col = lax.broadcasted_iota(jnp.int32, (C, W), 1)
    cold = lax.broadcasted_iota(jnp.int32, (C, 128), 1)
    diag = cold == lax.broadcasted_iota(jnp.int32, (C, 128), 0)

    def pick(value, lane):
        return jnp.sum(jnp.where(col == lane, value, 0.0), axis=1, keepdims=True)

    def spread(step, store, ssem, rsem):
        def one(k):
            _, who = peer(k)
            remote(store.at[step, me], store.at[step, me], ssem.at[step, k], rsem.at[step, me], who).start()

        each(G - 1, one)

    def gathered_sum(step, store, ssem, rsem, zero):
        def arrive(k):
            g, who = peer(k)
            remote(store.at[step, g], store.at[step, g], ssem.at[step, 0], rsem.at[step, g], who).wait_recv()

        each(G - 1, arrive)
        if G <= 8:
            total = store[step, 0]
            for g in range(1, G):
                total = total + store[step, g]
            return total
        return lax.fori_loop(0, G, lambda g, t: t + store[step, g], zero)

    def corners(step, z_left, z_right, r_left):
        for q in range(R):
            half = z_left if q < half_r else z_right
            at = (q % half_r) * B
            zs[q] = half[:, at : at + B]
        gamma = jnp.sum(r_left * z_left, axis=1, keepdims=True)
        gamma = jnp.where(r == 0, gamma, 0.0)
        corner = dot_nt(zs[r].astype(BF), mo[r])
        pk[step, me] = corner + jnp.where(col == NC, gamma, 0.0)
        spread(step, pk, pk_ssem, pk_rsem)

    def product(step, local):
        own[step, r] = local.astype(BF)
        delta = jnp.sum(zs[r] * local, axis=1, keepdims=True)
        dk[step, me] = jnp.sum(jnp.where(diag, delta, 0.0), axis=0, keepdims=True)
        spread(step, dk, dk_ssem, dk_rsem)
        mine = own.at[step, r]
        sends = [
            to_side(mine, nbr.at[step], nbr_ssem.at[step], nbr_rsem.at[step], (k + 1) % R) for k in range(R)
        ]
        sends += [
            to_row(mine, own.at[step], own_ssem.at[step], own_rsem.at[step], k) for k in range(1, R)
        ]
        for copy in sends:
            copy.start()
        return sends

    def solve(step):
        total = gathered_sum(step, pk, pk_ssem, pk_rsem, jnp.zeros((C, W), F32))
        solved = lax.dot_general(
            total, cinv_p[...], (((1,), (0,)), ((), ())),
            precision=lax.Precision.HIGHEST, preferred_element_type=F32,
        )
        back = solved.astype(BF)
        gamma = pick(total, NC)
        bend = jnp.sum(total * back.astype(F32), axis=1, keepdims=True)
        return back, gamma, bend

    def joined(store, first, last):
        return jnp.concatenate([store[q] for q in range(first, last)], axis=1)

    def bent(back, first, last):
        return jnp.concatenate(
            [dot_nn(back, mo[q]) + dot_nn(back, mn[q]) for q in range(first, last)], axis=1
        )

    def slope(step, bend):
        total = gathered_sum(step, dk, dk_ssem, dk_rsem, jnp.zeros((1, 128), F32))
        return jnp.sum(jnp.where(diag, total, 0.0), axis=1, keepdims=True) + bend

    def arrive(step):
        for k in range(1, R):
            wait_slot(own.at[step], own_ssem.at[step], own_rsem.at[step], lax.rem(r + k, R))
        for q in range(R):
            wait_slot(nbr.at[step], nbr_ssem.at[step], nbr_rsem.at[step], q)

    corners(0, z0, z0_r, r0)
    pl.when(s != S - 1)(send_maps)
    local0 = acc[...] + dot_nt(z0_r.astype(BF), op_v[:, H:])
    sends0 = product(0, local0)

    for k in range(1, R):
        q = lax.rem(r + k, R)
        wait_slot(cmo, cmo_ssem, cmo_rsem, q)
        mo[q] = dot_nn(hot_own, cmo[q]).astype(BF)
    hot_next = hot_ids(nxt)
    hot_prev = hot_ids(prv)
    for q in range(R):
        wait_slot(cmn, cmn_ssem, cmn_rsem, q)
        mn[q] = dot_nn(hot_next if q < half_r else hot_prev, cmn[q]).astype(BF)
    right = dot_nn(joined(mn, 0, half_r), pr_m[...]).astype(BF)
    left = dot_nn(joined(mn, half_r, R), pl_m[...]).astype(BF)
    for q in range(R):
        at = (q % half_r) * B
        mn[q] = (left if q < half_r else right)[:, at : at + B]

    back0, gamma0, bend0 = solve(0)
    fix_l = bent(back0, 0, half_r)
    fix_r = bent(back0, half_r, R)
    delta0 = slope(0, bend0)
    alpha0 = gamma0 / delta0
    arrive(0)
    wr0 = (joined(own[0], half_r, R).astype(F32) + fix_r + dot_nn(joined(nbr[0], 0, half_r), pr_m[...])) * live_r
    wl0 = (joined(own[0], 0, half_r).astype(F32) + fix_l + dot_nn(joined(nbr[0], half_r, R), pl_m[...])) * live_l
    r1 = r0 - alpha0 * wl0
    z1 = w_l * r1
    z1_r = z0_r - alpha0 * (w_r * wr0)
    corners(1, z1, z1_r, r1)
    local1 = dot_nt(jnp.concatenate([z1.astype(BF), z1_r.astype(BF)], axis=1), op_v[...])
    sends1 = product(1, local1)
    back1, gamma1, bend1 = solve(1)
    fix = bent(back1, 0, half_r)
    beta = gamma1 / gamma0
    delta1 = slope(1, bend1)
    alpha1 = gamma1 / (delta1 - beta * gamma1 / alpha0)
    sol[...] = alpha0 * z0 + alpha1 * (z1 + beta * z0)
    arrive(1)
    wl1 = (joined(own[1], 0, half_r).astype(F32) + fix + dot_nn(joined(nbr[1], half_r, R), pl_m[...])) * live_l
    res[...] = r1 - alpha1 * (wl1 + beta * wl0)

    z_copy.wait_send()
    w_copy.wait_send()
    for copy in cm_sends + sends0 + sends1:
        copy.wait_send()
    for step in range(2):

        def drain(k):
            _, who = peer(k)
            for store, ssem, rsem in ((pk, pk_ssem, pk_rsem), (dk, dk_ssem, dk_rsem)):
                remote(
                    store.at[step, me], store.at[step, me], ssem.at[step, k], rsem.at[step, me], who
                ).wait_send()

        each(G - 1, drain)


def finish(a, b, x, y, sem):
    first = pltpu.make_async_copy(a, x.at[0], sem.at[0])
    second = pltpu.make_async_copy(b, y.at[0], sem.at[1])
    first.start()
    second.start()
    first.wait()
    second.wait()


def per_device(S, R, loads, weights, dual_ops, corner_maps, coarse_inverse, corner_ids,
               iface_sizes, left_partner, right_partner):
    _, C, H = loads.shape
    _, B, full = dual_ops.shape
    J = corner_maps.shape[1]
    NC = coarse_inverse.shape[0]
    W = (NC + 1 + 127) // 128 * 128
    G = S * R
    DMA = pltpu.SemaphoreType.DMA
    hbm = pl.BlockSpec(memory_space=pltpu.HBM)
    vmem = pl.BlockSpec(memory_space=pltpu.VMEM)
    given = [
        pltpu.with_memory_space_constraint(x, pltpu.HBM)
        for x in (loads, weights, dual_ops, corner_maps, coarse_inverse, corner_ids, iface_sizes,
                  left_partner, right_partner)
    ]
    held = pltpu.VMEM((C, H), F32)
    made = pl.pallas_call(
        functools.partial(kernel, S, R),
        out_shape=(held, held),
        in_specs=[hbm] * 9,
        out_specs=(vmem, vmem),
        scratch_shapes=[
            pltpu.VMEM((C, H), F32), pltpu.VMEM((1, H), F32), pltpu.VMEM((B, full), BF),
            pltpu.VMEM((NC, NC), F32), pltpu.VMEM((W, W), F32), pltpu.VMEM(corner_ids.shape, jnp.int32),
            pltpu.VMEM((1, H), jnp.int32), pltpu.VMEM((1, H), jnp.int32), pltpu.SMEM(iface_sizes.shape, jnp.int32),
            pltpu.VMEM((C, H), BF), pltpu.VMEM((C, H), BF), pltpu.VMEM((1, H), F32),
            pltpu.VMEM((R, J, B), BF), pltpu.VMEM((R, J, B), BF),
            pltpu.VMEM((R, W, B), BF), pltpu.VMEM((R, W, B), BF),
            pltpu.VMEM((H, H), BF), pltpu.VMEM((H, H), BF), pltpu.VMEM((R, C, B), F32), pltpu.VMEM((C, B), F32),
            pltpu.VMEM((2, R, C, B), BF), pltpu.VMEM((2, R, C, B), BF), pltpu.VMEM((2, G, C, W), F32),
            pltpu.VMEM((2, G, 1, 128), F32),
            DMA((8,)), DMA, DMA((4,)), DMA((R,)), DMA((R,)), DMA((R,)), DMA((R,)),
            DMA((2, R)), DMA((2, R)), DMA((2, R)), DMA((2, R)), DMA((2, G)), DMA((2, G)), DMA((2, G)), DMA((2, G)),
        ],
        compiler_params=pltpu.CompilerParams(
            collective_id=0, has_side_effects=True, vmem_limit_bytes=LIMIT
        ),
    )(*given)
    done = jax.ShapeDtypeStruct((1, C, H), F32)
    return pl.pallas_call(
        finish,
        out_shape=(done, done),
        in_specs=[vmem] * 2,
        out_specs=(hbm, hbm),
        scratch_shapes=[DMA((2,))],
        compiler_params=pltpu.CompilerParams(vmem_limit_bytes=2**20),
    )(*[pltpu.with_memory_space_constraint(x, pltpu.VMEM) for x in made])


def solution(mesh):
    placed = (
        P(("parts", "sub"), "col", None),
        P(("parts", "sub"), None),
        P(("parts", "sub"), "row", None),
        P(("parts", "sub"), None, "row"),
        P("parts", None),
        P("parts", None),
        P("parts"),
        P(("parts", "sub"), None),
        P(("parts", "sub"), None),
    )
    return jax.shard_map(
        functools.partial(per_device, mesh.shape["sub"], mesh.shape["row"]),
        mesh=mesh,
        in_specs=placed,
        out_specs=(P(("parts", "sub"), "col", None), P(("parts", "sub"), "col", None)),
        check_vma=False,
    )
```

```python
import functools

import jax
import jax.numpy as jnp
from jax import lax
from jax.experimental import pallas as pl
from jax.experimental.pallas import tpu as pltpu
from jax.sharding import PartitionSpec as P

MESH = pl.DeviceIdType.MESH
LIMIT = 40 * 2**20
BF = jnp.bfloat16
F32 = jnp.float32


def each(count, body):
    if count <= 8:
        for at in range(count):
            body(at)
    else:
        lax.fori_loop(0, count, lambda at, _: (body(at), 0)[1], 0)


def dot_nt(a, b):
    return lax.dot_general(a, b, (((1,), (1,)), ((), ())), preferred_element_type=F32)


def dot_nn(a, b):
    return lax.dot_general(a, b, (((1,), (0,)), ((), ())), preferred_element_type=F32)


def kernel(
    S, R, loads, weights, op, cm, cinv, ids, sizes, lmap, rmap, sol, res,
    loads_v, w_v, op_v, cv, cinv_p, ids_v, lmap_v, rmap_v, sizes_v,
    zsend, zrecv, wrecv, cm_v, cmo, cmn, mm, hots, zs, acc, turned, zz, wt, live, fixed, met, sol_v, res_v,
    blocks, pk, dk,
    in_sem, op_sem, z_sem, cmo_ssem, cmo_rsem, cmn_ssem, cmn_rsem,
    blk_ssem, own_rsem, nbr_rsem, pk_ssem, pk_rsem, dk_ssem, dk_rsem, out_sem,
):
    s = lax.axis_index("sub")
    r = lax.axis_index("row")
    G = S * R
    me = s * R + r
    C, H = loads_v.shape
    B = op_v.shape[0]
    NC = cv.shape[0]
    W = cinv_p.shape[0]
    half_r = R // 2
    nxt = lax.rem(s + 1, S)
    prv = lax.rem(s + S - 1, S)
    side = r // half_r
    toward = lax.rem(s + S - 1 + 2 * side, S)

    barrier = pltpu.get_barrier_semaphore()

    def peer(k):
        g = lax.rem(me + k + 1, G)
        return g, {"sub": g // R, "row": lax.rem(g, R)}

    def greet(k):
        _, who = peer(k)
        pl.semaphore_signal(barrier, inc=1, device_id=who, device_id_type=MESH)

    each(G - 1, greet)

    ins = [
        pltpu.make_async_copy(src, dst, in_sem.at[i])
        for i, (src, dst) in enumerate([
            (loads.at[0], loads_v), (weights, w_v), (sizes, sizes_v), (rmap, rmap_v), (lmap, lmap_v),
            (ids, ids_v), (cinv, cv), (cm.at[0], cm_v),
        ])
    ]
    for copy in ins:
        copy.start()
    op_copy = pltpu.make_async_copy(op.at[0], op_v, op_sem)
    op_copy.start()

    for copy in ins[:3]:
        copy.wait()
    lanes = lax.broadcasted_iota(jnp.int32, (1, H), 1)
    live_l = (lanes < sizes_v[prv]).astype(F32)
    live[0] = live_l
    size_after = sizes_v[s]
    w_l = w_v[...]
    r0 = loads_v[...] * live_l
    z0 = w_l * r0
    zsend[...] = z0.astype(BF)
    zz[0] = z0
    wt[0] = w_l

    ins[7].wait()
    J = cm_v.shape[0]
    J0 = cmo.shape[1]
    own_map = cm_v[...].astype(F32)
    if J0 < J:
        tail = own_map[J0:]
        folded = jnp.concatenate([tail[:, : B // 2], tail[:, B // 2 :]], axis=0)
        cmo[r] = jnp.concatenate([own_map[:J0], folded], axis=1).astype(BF)
    else:
        cmo[r] = own_map.astype(BF)

    def spreadout(hot, kept):
        if J0 == J:
            return dot_nn(hot, kept)
        tail = kept[:, B:].astype(F32)
        lower = jnp.concatenate([tail[: J - J0], tail[J - J0 :]], axis=1)
        return dot_nn(hot, jnp.concatenate([kept[:, :B].astype(F32), lower], axis=0).astype(BF))

    pl.semaphore_wait(barrier, G - 1)

    def remote(src, dst, ssem, rsem, who):
        return pltpu.make_async_remote_copy(
            src_ref=src, dst_ref=dst, send_sem=ssem, recv_sem=rsem, device_id=who, device_id_type=MESH
        )

    z_copy = remote(zsend, zrecv, z_sem.at[0], z_sem.at[1], {"sub": prv})
    w_copy = remote(w_v, wrecv, z_sem.at[2], z_sem.at[3], {"sub": prv})
    z_copy.start()
    w_copy.start()

    def to_row(src, dst, ssem, rsem, k):
        return remote(src, dst.at[r], ssem, rsem, {"row": lax.rem(r + k, R)})

    def to_side(src, dst, ssem, rsem, k):
        return remote(src, dst.at[r], ssem, rsem, {"sub": toward, "row": lax.rem(r + k, R)})

    def wait_slot(dst, rsem, q):
        remote(dst.at[q], dst.at[q], rsem, rsem, {"sub": nxt}).wait_recv()

    cm_sides = [to_side(cmo.at[r], cmn, cmn_ssem.at[k], cmn_rsem.at[k], k) for k in range(R)]
    cm_rows = [to_row(cmo.at[r], cmo, cmo_ssem.at[k - 1], cmo_rsem.at[k - 1], k) for k in range(1, R)]
    for copy in cm_rows + cm_sides[:1]:
        copy.start()

    ins[3].wait()
    ins[4].wait()
    right_map = rmap_v[...]
    left_map = lmap_v[...]
    live[1] = (right_map < size_after).astype(F32)

    def hot(target, the_map):
        step = 128
        for c in range(H // step):
            rows = lax.broadcasted_iota(jnp.int32, (step, H), 0) + c * step
            target[pl.ds(c * step, step), :] = (rows == the_map).astype(F32).astype(BF)

    hot(hots.at[1], right_map)
    hot(hots.at[0], left_map)
    ins[5].wait()
    ins[6].wait()
    cinv_p[...] = jnp.zeros_like(cinv_p)
    cinv_p[0:NC, 0:NC] = cv[...]

    def hot_ids(t):
        row = ids_v[pl.ds(t, 1), :]
        rows = lax.broadcasted_iota(jnp.int32, (W, row.shape[1]), 0)
        return (rows == row).astype(F32).astype(BF)

    hot_own = hot_ids(s)
    mm[r, 0:W] = spreadout(hot_own, cmo[r]).astype(BF)

    op_copy.wait()
    step = 256
    for c in range(2 * H // step):
        turned[c * step // H, c * step % H : c * step % H + step, :] = op_v[:, c * step : (c + 1) * step].T
    acc[...] = dot_nn(z0.astype(BF), turned[0])

    for copy in cm_sides[1:]:
        copy.start()
    z_copy.wait_recv()
    w_copy.wait_recv()
    w_in = wrecv[...]
    w_hi = w_in.astype(BF)
    w_lo = (w_in - w_hi.astype(F32)).astype(BF)
    pad = lax.broadcasted_iota(jnp.int32, (16, H), 0)
    w_rows = jnp.where(pad == 0, w_hi.astype(F32), jnp.where(pad == 1, w_lo.astype(F32), 0.0))
    gathered = dot_nn(jnp.concatenate([zrecv[...], w_rows.astype(BF)], axis=0), hots[1])
    z0_r = gathered[:C]
    zz[1] = z0_r
    wt[1] = gathered[C : C + 1] + gathered[C + 1 : C + 2]

    col = lax.broadcasted_iota(jnp.int32, (C, W), 1)
    cold = lax.broadcasted_iota(jnp.int32, (C, 128), 1)
    diag = cold == lax.broadcasted_iota(jnp.int32, (C, 128), 0)

    def pick(value, lane):
        return jnp.sum(jnp.where(col == lane, value, 0.0), axis=1, keepdims=True)

    fold = C == 16 and W == 128 and NC < 64

    def packed(value):
        return value[:8] + pltpu.roll(value[8:], 64, 1) if fold else value

    def unpacked(value):
        if not fold:
            return value
        low = lax.broadcasted_iota(jnp.int32, value.shape, 1) < 64
        return jnp.concatenate(
            [jnp.where(low, value, 0.0), pltpu.roll(jnp.where(low, 0.0, value), 64, 1)], axis=0
        )

    def spread(step, store, ssem, rsem):
        def one(k):
            _, who = peer(k)
            remote(store.at[step, me], store.at[step, me], ssem.at[step], rsem.at[step], who).start()

        each(G - 1, one)

    def gathered_sum(step, store, ssem, rsem, zero):
        rest = store.at[step, pl.ds(0, G - 1)]
        remote(rest, rest, ssem.at[step], rsem.at[step], {"sub": nxt}).wait_recv()
        if G <= 8:
            total = store[step, 0]
            for g in range(1, G):
                total = total + store[step, g]
            return total
        return lax.fori_loop(0, G, lambda g, t: t + store[step, g], zero)

    def split(d, z):
        for j in range(half_r):
            zs[d * half_r + j] = z[:, j * B : (j + 1) * B]

    def corners(step, r_left, z_left):
        gamma = jnp.sum(r_left * z_left, axis=1, keepdims=True)
        gamma = jnp.where(r == 0, gamma, 0.0)
        corner = dot_nt(zs[r].astype(BF), mm[r, 0:W])
        pk[step, me] = packed(corner + jnp.where(col == NC, gamma, 0.0))
        spread(step, pk, pk_ssem, pk_rsem)

    def product(step, local):
        blocks[step, r] = local.astype(BF)
        mine = blocks.at[step, r]
        delta = jnp.sum(zs[r] * local, axis=1, keepdims=True)
        dk[step, me] = jnp.sum(jnp.where(diag, delta, 0.0), axis=0, keepdims=True)
        spread(step, dk, dk_ssem, dk_rsem)
        nbr = blocks.at[step, pl.ds(R, R)]
        sides = [to_side(mine, nbr, blk_ssem.at[step], nbr_rsem.at[step, k], k) for k in range(R)]
        rows = [to_row(mine, blocks.at[step], blk_ssem.at[step], own_rsem.at[step, k - 1], k) for k in range(1, R)]

        def start(copies):
            for copy in copies:
                copy.start()

        if step == 0:
            start(rows + sides)
        else:
            pl.when(side == 0)(lambda: start(rows))
            pl.when(side == 1)(lambda: start(sides[1:] + sides[:1]))

    def solve(step):
        total = unpacked(gathered_sum(step, pk, pk_ssem, pk_rsem, jnp.zeros(pk.shape[2:], F32)))
        solved = lax.dot_general(
            total, cinv_p[...], (((1,), (0,)), ((), ())),
            precision=lax.Precision.HIGHEST, preferred_element_type=F32,
        )
        back = solved.astype(BF)
        gamma = pick(total, NC)
        bend = jnp.sum(total * back.astype(F32), axis=1, keepdims=True)
        return back, gamma, bend

    def bent(back, first, last):
        twice = jnp.concatenate([back, back], axis=1)
        return jnp.concatenate([dot_nn(twice, mm[q]) for q in range(first, last)], axis=1)

    def slope(step, total, bend):
        return jnp.sum(jnp.where(diag, total, 0.0), axis=1, keepdims=True) + bend

    def meet_own(step):
        for k in range(1, R):
            q = lax.rem(r + R - k, R)
            take = functools.partial(wait_slot, blocks.at[step], own_rsem.at[step, k - 1], q)
            if step == 0:
                take()
            else:
                pl.when(q < half_r)(take)

    def meet(step, d):
        for j in range(half_r):
            q = (1 - d) * half_r + j
            wait_slot(blocks.at[step], nbr_rsem.at[step, lax.rem(r - q + R, R)], R + q)

    def meeting(step, d):
        start = (1 - d) * half_r
        theirs = jnp.concatenate([blocks[step, R + start + j] for j in range(half_r)], axis=1)
        mine = jnp.concatenate([blocks[step, d * half_r + j] for j in range(half_r)], axis=1)
        return mine.astype(F32) + dot_nn(theirs, hots[d])

    split(0, z0)
    split(1, z0_r)
    corners(0, r0, z0)
    local0 = acc[...] + dot_nn(z0_r.astype(BF), turned[1])
    product(0, local0)

    for k in range(1, R):
        q = lax.rem(r + R - k, R)
        wait_slot(cmo, cmo_rsem.at[k - 1], q)
        mm[q, 0:W] = spreadout(hot_own, cmo[q]).astype(BF)
    hot_next = hot_ids(nxt)
    hot_prev = hot_ids(prv)
    for k in range(R):
        wait_slot(cmn, cmn_rsem.at[k], lax.rem(r + R - k, R))
    for q in range(R):
        mm[q, W : 2 * W] = spreadout(hot_next if q < half_r else hot_prev, cmn[q]).astype(BF)
    right = dot_nn(jnp.concatenate([mm[q, W : 2 * W] for q in range(half_r)], axis=1), hots[1]).astype(BF)
    left = dot_nn(jnp.concatenate([mm[q, W : 2 * W] for q in range(half_r, R)], axis=1), hots[0]).astype(BF)
    for q in range(R):
        at = (q % half_r) * B
        mm[q, W : 2 * W] = (left if q < half_r else right)[:, at : at + B]

    early = jnp.where(s == 0, 1, 0)
    late = 1 - early
    meet_own(0)
    meet(0, early)
    met[early] = meeting(0, early)
    back0, gamma0, bend0 = solve(0)
    fixed[0] = bent(back0, 0, half_r)
    fixed[1] = bent(back0, half_r, R)
    steep0 = gathered_sum(0, dk, dk_ssem, dk_rsem, jnp.zeros((1, 128), F32))
    meet(0, late)
    delta0 = slope(0, steep0, bend0)
    alpha0 = gamma0 / delta0

    def advance(d):
        met[d] = (met[d] + fixed[d]) * live[d]
        z = zz[d] - alpha0 * (wt[d] * met[d])
        split(d, z)
        return z.astype(BF)

    met[late] = meeting(0, late)
    acc[...] = dot_nn(advance(early), turned[early])
    last = advance(late)
    wl0 = met[0]
    r1 = r0 - alpha0 * wl0
    z1 = jnp.concatenate([zs[q] for q in range(half_r)], axis=1)
    corners(1, r1, z1)
    local1 = acc[...] + dot_nn(last, turned[late])
    product(1, local1)
    back1, gamma1, bend1 = solve(1)
    fix = bent(back1, 0, half_r)
    beta = gamma1 / gamma0
    steep1 = gathered_sum(1, dk, dk_ssem, dk_rsem, jnp.zeros((1, 128), F32))
    meet_own(1)
    meet(1, 0)
    delta1 = slope(1, steep1, bend1)
    alpha1 = gamma1 / (delta1 - beta * gamma1 / alpha0)
    sol_v[...] = alpha0 * z0 + alpha1 * (z1 + beta * z0)
    sol_out = pltpu.make_async_copy(sol_v, sol, out_sem.at[0])
    sol_out.start()
    wl1 = (meeting(1, 0) + fix) * live[0]
    res_v[...] = r1 - alpha1 * (wl1 + beta * wl0)
    res_out = pltpu.make_async_copy(res_v, res, out_sem.at[1])
    res_out.start()

    z_copy.wait_send()
    w_copy.wait_send()
    for copy in cm_sides + cm_rows:
        copy.wait_send()
    for step in range(2):
        def sent(count):
            gone = blocks.at[step, pl.ds(0, count)]
            remote(gone, gone, blk_ssem.at[step], blk_ssem.at[step], {"sub": nxt}).wait_send()

        if step == 0:
            sent(2 * R - 1)
        else:
            pl.when(side == 0)(functools.partial(sent, R - 1))
            pl.when(side == 1)(functools.partial(sent, R))
        for store, ssem, rsem in ((pk, pk_ssem, pk_rsem), (dk, dk_ssem, dk_rsem)):
            rest = store.at[step, pl.ds(0, G - 1)]
            remote(rest, rest, ssem.at[step], rsem.at[step], {"sub": nxt}).wait_send()
    sol_out.wait()
    res_out.wait()


def finish(a, b, x, y, sem):
    first = pltpu.make_async_copy(a, x.at[0], sem.at[0])
    second = pltpu.make_async_copy(b, y.at[0], sem.at[1])
    first.start()
    second.start()
    first.wait()
    second.wait()


def per_device(S, R, loads, weights, dual_ops, corner_maps, coarse_inverse, corner_ids,
               iface_sizes, left_partner, right_partner):
    _, C, H = loads.shape
    _, B, full = dual_ops.shape
    J = corner_maps.shape[1]
    NC = coarse_inverse.shape[0]
    W = (NC + 1 + 127) // 128 * 128
    G = S * R
    fold = (16 * (J // 16), B + B // 2) if J % 16 == 8 and J < 32 else (J, B)
    DMA = pltpu.SemaphoreType.DMA
    hbm = pl.BlockSpec(memory_space=pltpu.HBM)
    vmem = pl.BlockSpec(memory_space=pltpu.VMEM)
    given = [
        pltpu.with_memory_space_constraint(x, pltpu.HBM)
        for x in (loads, weights, dual_ops, corner_maps, coarse_inverse, corner_ids, iface_sizes,
                  left_partner, right_partner)
    ]
    held = pltpu.VMEM((C, H), F32)
    made = pl.pallas_call(
        functools.partial(kernel, S, R),
        out_shape=(held, held),
        in_specs=[hbm] * 9,
        out_specs=(pl.BlockSpec(memory_space=pl.ANY),) * 2,
        scratch_shapes=[
            pltpu.VMEM((C, H), F32), pltpu.VMEM((1, H), F32), pltpu.VMEM((B, full), BF),
            pltpu.VMEM((NC, NC), F32), pltpu.VMEM((W, W), F32), pltpu.VMEM(corner_ids.shape, jnp.int32),
            pltpu.VMEM((1, H), jnp.int32), pltpu.VMEM((1, H), jnp.int32), pltpu.SMEM(iface_sizes.shape, jnp.int32),
            pltpu.VMEM((C, H), BF), pltpu.VMEM((C, H), BF), pltpu.VMEM((1, H), F32),
            pltpu.VMEM((J, B), BF), pltpu.VMEM((R,) + fold, BF), pltpu.VMEM((R,) + fold, BF),
            pltpu.VMEM((R, 2 * W, B), BF),
            pltpu.VMEM((2, H, H), BF), pltpu.VMEM((R, C, B), F32), pltpu.VMEM((C, B), F32),
            pltpu.VMEM((2, H, B), BF), pltpu.VMEM((2, C, H), F32), pltpu.VMEM((2, 1, H), F32), pltpu.VMEM((2, 1, H), F32),
            pltpu.VMEM((2, C, H), F32), pltpu.VMEM((2, C, H), F32), pltpu.VMEM((C, H), F32), pltpu.VMEM((C, H), F32),
            pltpu.VMEM((2, 2 * R, C, B), BF), pltpu.VMEM((2, G, 8 if C == 16 and W == 128 and NC < 64 else C, W), F32),
            pltpu.VMEM((2, G, 1, 128), F32),
            DMA((8,)), DMA, DMA((4,)), DMA((R - 1,)), DMA((R - 1,)), DMA((R,)), DMA((R,)),
            DMA((2,)), DMA((2, R - 1)), DMA((2, R)), DMA((2,)), DMA((2,)), DMA((2,)), DMA((2,)), DMA((2,)),
        ],
        compiler_params=pltpu.CompilerParams(
            collective_id=0, has_side_effects=True, vmem_limit_bytes=LIMIT
        ),
    )(*given)
    done = jax.ShapeDtypeStruct((1, C, H), F32)
    return pl.pallas_call(
        finish,
        out_shape=(done, done),
        in_specs=[vmem] * 2,
        out_specs=(hbm, hbm),
        scratch_shapes=[DMA((2,))],
        compiler_params=pltpu.CompilerParams(vmem_limit_bytes=2**20),
    )(*[pltpu.with_memory_space_constraint(x, pltpu.VMEM) for x in made])


def solution(mesh):
    placed = (
        P(("parts", "sub"), "col", None),
        P(("parts", "sub"), None),
        P(("parts", "sub"), "row", None),
        P(("parts", "sub"), None, "row"),
        P("parts", None),
        P("parts", None),
        P("parts"),
        P(("parts", "sub"), None),
        P(("parts", "sub"), None),
    )
    return jax.shard_map(
        functools.partial(per_device, mesh.shape["sub"], mesh.shape["row"]),
        mesh=mesh,
        in_specs=placed,
        out_specs=(P(("parts", "sub"), "col", None), P(("parts", "sub"), "col", None)),
        check_vma=False,
    )
```

```python
import functools

import jax
import jax.numpy as jnp
from jax import lax
from jax.experimental import pallas as pl
from jax.experimental.pallas import tpu as pltpu
from jax.sharding import PartitionSpec as P

MESH = pl.DeviceIdType.MESH
LIMIT = 40 * 2**20
BF = jnp.bfloat16
F32 = jnp.float32


def each(count, body):
    if count <= 8:
        for at in range(count):
            body(at)
    else:
        lax.fori_loop(0, count, lambda at, _: (body(at), 0)[1], 0)


def dot_nt(a, b):
    return lax.dot_general(a, b, (((1,), (1,)), ((), ())), preferred_element_type=F32)


def dot_nn(a, b):
    return lax.dot_general(a, b, (((1,), (0,)), ((), ())), preferred_element_type=F32)


def kernel(
    S, R, loads, weights, op, cm, cinv, ids, sizes, lmap, rmap, sol, res,
    loads_v, w_v, op_v, cv, cinv_p, ids_v, lmap_v, rmap_v, sizes_v,
    zsend, zrecv, wrecv, cm_v, cmo, cmn, mm, hots, zs, acc, turned, zz, wt, live, fixed, met,
    blocks, pk, dk,
    in_sem, op_sem, z_sem, cmo_ssem, cmo_rsem, cmn_ssem, cmn_rsem,
    blk_ssem, own_rsem, nbr_rsem, pk_ssem, pk_rsem, dk_ssem, dk_rsem, ready,
):
    s = lax.axis_index("sub")
    r = lax.axis_index("row")
    G = S * R
    me = s * R + r
    C, H = loads_v.shape
    B = op_v.shape[0]
    NC = cv.shape[0]
    W = cinv_p.shape[0]
    half_r = R // 2
    nxt = lax.rem(s + 1, S)
    prv = lax.rem(s + S - 1, S)
    side = r // half_r
    toward = lax.rem(s + S - 1 + 2 * side, S)

    barrier = pltpu.get_barrier_semaphore()

    def peer(k):
        g = lax.rem(me + k + 1, G)
        return g, {"sub": g // R, "row": lax.rem(g, R)}

    def greet(k):
        _, who = peer(k)
        pl.semaphore_signal(barrier, inc=1, device_id=who, device_id_type=MESH)

    def tell(semaphore, k):
        pl.semaphore_signal(
            semaphore, inc=1, device_id={"row": lax.rem(r + k, R)}, device_id_type=MESH
        )

    close = S <= 4
    if close:
        for other in (nxt, prv) if S > 2 else (nxt,):
            pl.semaphore_signal(barrier, inc=1, device_id={"sub": other}, device_id_type=MESH)
        for k in range(1, R):
            tell(barrier, k)
        met_first = (2 if S > 2 else 1) + R - 1
    else:
        each(G - 1, greet)
        met_first = G - 1

    ins = [
        pltpu.make_async_copy(src, dst, in_sem.at[i])
        for i, (src, dst) in enumerate([
            (loads.at[0], loads_v), (weights, w_v), (sizes, sizes_v), (rmap, rmap_v), (lmap, lmap_v),
            (ids, ids_v), (cinv, cv), (cm.at[0], cm_v),
        ])
    ]
    for copy in ins:
        copy.start()
    op_copy = pltpu.make_async_copy(op.at[0], op_v, op_sem)
    op_copy.start()

    for copy in ins[:3]:
        copy.wait()
    lanes = lax.broadcasted_iota(jnp.int32, (1, H), 1)
    live_l = (lanes < sizes_v[prv]).astype(F32)
    live[0] = live_l
    size_after = sizes_v[s]
    w_l = w_v[...]
    r0 = loads_v[...] * live_l
    z0 = w_l * r0
    zsend[...] = z0.astype(BF)
    zz[0] = z0
    wt[0] = w_l

    ins[7].wait()
    J = cm_v.shape[0]
    J0 = cmo.shape[1]
    own_map = cm_v[...].astype(F32)
    if J0 < J:
        tail = own_map[J0:]
        folded = jnp.concatenate([tail[:, : B // 2], tail[:, B // 2 :]], axis=0)
        cmo[r] = jnp.concatenate([own_map[:J0], folded], axis=1).astype(BF)
    else:
        cmo[r] = own_map.astype(BF)

    def spreadout(hot, kept):
        if J0 == J:
            return dot_nn(hot, kept)
        tail = kept[:, B:].astype(F32)
        lower = jnp.concatenate([tail[: J - J0], tail[J - J0 :]], axis=1)
        return dot_nn(hot, jnp.concatenate([kept[:, :B].astype(F32), lower], axis=0).astype(BF))

    pl.semaphore_wait(barrier, met_first)

    def remote(src, dst, ssem, rsem, who):
        return pltpu.make_async_remote_copy(
            src_ref=src, dst_ref=dst, send_sem=ssem, recv_sem=rsem, device_id=who, device_id_type=MESH
        )

    z_copy = remote(zsend, zrecv, z_sem.at[0], z_sem.at[1], {"sub": prv})
    w_copy = remote(w_v, wrecv, z_sem.at[2], z_sem.at[3], {"sub": prv})
    z_copy.start()
    w_copy.start()
    for k in range(1, R):
        tell(ready.at[0], k)

    def to_row(src, dst, ssem, rsem, k):
        return remote(src, dst.at[r], ssem, rsem, {"row": lax.rem(r + k, R)})

    def to_side(src, dst, ssem, rsem, k):
        return remote(src, dst.at[r], ssem, rsem, {"sub": toward, "row": lax.rem(r + k, R)})

    def wait_slot(dst, rsem, q):
        remote(dst.at[q], dst.at[q], rsem, rsem, {"sub": nxt}).wait_recv()

    cm_sides = [to_side(cmo.at[r], cmn, cmn_ssem.at[k], cmn_rsem.at[k], k) for k in range(R)]
    cm_rows = [to_row(cmo.at[r], cmo, cmo_ssem.at[k - 1], cmo_rsem.at[k - 1], k) for k in range(1, R)]
    def launch(copies):
        for copy in copies:
            copy.start()

    far = jnp.logical_or(s == 0, s == S - 1)
    launch(cm_sides[:1])
    launch(cm_rows)

    ins[3].wait()
    ins[4].wait()
    right_map = rmap_v[...]
    left_map = lmap_v[...]
    live[1] = (right_map < size_after).astype(F32)

    def hot(target, the_map):
        step = 128
        for c in range(H // step):
            rows = lax.broadcasted_iota(jnp.int32, (step, H), 0) + c * step
            target[pl.ds(c * step, step), :] = (rows == the_map).astype(F32).astype(BF)

    hot(hots.at[1], right_map)
    hot(hots.at[0], left_map)
    ins[5].wait()
    ins[6].wait()
    cinv_p[...] = jnp.zeros_like(cinv_p)
    cinv_p[0:NC, 0:NC] = cv[...]

    pl.semaphore_wait(ready.at[0], R - 1)
    pl.when(far)(lambda: launch(cm_sides[1:]))

    def hot_ids(t):
        row = ids_v[pl.ds(t, 1), :]
        rows = lax.broadcasted_iota(jnp.int32, (W, row.shape[1]), 0)
        return (rows == row).astype(F32).astype(BF)

    hot_own = hot_ids(s)
    mm[r, 0:W] = spreadout(hot_own, cmo[r]).astype(BF)

    op_copy.wait()
    step = 256
    for c in range(2 * H // step):
        turned[c * step // H, c * step % H : c * step % H + step, :] = op_v[:, c * step : (c + 1) * step].T
    acc[...] = dot_nn(z0.astype(BF), turned[0])

    for k in range(1, R):
        q = lax.rem(r + R - k, R)
        wait_slot(cmo, cmo_rsem.at[k - 1], q)
        mm[q, 0:W] = spreadout(hot_own, cmo[q]).astype(BF)
    pl.when(jnp.logical_not(far))(lambda: launch(cm_sides[1:]))
    z_copy.wait_recv()
    w_copy.wait_recv()
    for k in range(1, R):
        tell(ready.at[1], k)
    w_in = wrecv[...]
    w_hi = w_in.astype(BF)
    w_lo = (w_in - w_hi.astype(F32)).astype(BF)
    pad = lax.broadcasted_iota(jnp.int32, (16, H), 0)
    w_rows = jnp.where(pad == 0, w_hi.astype(F32), jnp.where(pad == 1, w_lo.astype(F32), 0.0))
    gathered = dot_nn(jnp.concatenate([zrecv[...], w_rows.astype(BF)], axis=0), hots[1])
    z0_r = gathered[:C]
    zz[1] = z0_r
    wt[1] = gathered[C : C + 1] + gathered[C + 1 : C + 2]

    col = lax.broadcasted_iota(jnp.int32, (C, W), 1)
    cold = lax.broadcasted_iota(jnp.int32, (C, 128), 1)
    diag = cold == lax.broadcasted_iota(jnp.int32, (C, 128), 0)

    def pick(value, lane):
        return jnp.sum(jnp.where(col == lane, value, 0.0), axis=1, keepdims=True)

    fold = C == 16 and W == 128 and NC < 64

    def packed(value):
        return value[:8] + pltpu.roll(value[8:], 64, 1) if fold else value

    def unpacked(value):
        if not fold:
            return value
        low = lax.broadcasted_iota(jnp.int32, value.shape, 1) < 64
        return jnp.concatenate(
            [jnp.where(low, value, 0.0), pltpu.roll(jnp.where(low, 0.0, value), 64, 1)], axis=0
        )

    def spread(step, store, ssem, rsem):
        count = store.shape[1]
        slot = me if count == G else s

        def one(k):
            who = peer(k)[1] if count == G else {"sub": lax.rem(s + k + 1, S)}
            remote(store.at[step, slot], store.at[step, slot], ssem.at[step], rsem.at[step], who).start()

        each(count - 1, one)

    def gathered_sum(step, store, ssem, rsem, zero):
        count = store.shape[1]
        rest = store.at[step, pl.ds(0, count - 1)]
        remote(rest, rest, ssem.at[step], rsem.at[step], {"sub": nxt}).wait_recv()
        if count <= 8:
            total = store[step, 0]
            for g in range(1, count):
                total = total + store[step, g]
            return total
        return lax.fori_loop(0, count, lambda g, t: t + store[step, g], zero)

    def split(d, z):
        for j in range(half_r):
            zs[d * half_r + j] = z[:, j * B : (j + 1) * B]

    def product(step, local, r_left, z_left):
        blocks[step, r] = local.astype(BF)
        mine = blocks.at[step, r]
        delta = jnp.sum(zs[r] * local, axis=1, keepdims=True)
        dk[step, me] = jnp.sum(jnp.where(diag, delta, 0.0), axis=0, keepdims=True)
        gamma = jnp.sum(r_left * z_left, axis=1, keepdims=True)
        corner = jnp.where(col == NC, gamma, 0.0)
        for q in range(R):
            corner = corner + dot_nt(zs[q].astype(BF), mm[q, 0:W])
        pk[step, s] = packed(corner)
        nbr = blocks.at[step, pl.ds(R, R)]
        sides = [to_side(mine, nbr, blk_ssem.at[step], nbr_rsem.at[step, k], k) for k in range(R)]
        rows = [to_row(mine, blocks.at[step], blk_ssem.at[step], own_rsem.at[step, k - 1], k) for k in range(1, R)]

        spread(step, pk, pk_ssem, pk_rsem)
        if step == 0:
            launch(rows)
        else:
            pl.when(side == 0)(lambda: launch(rows))
        if step == 0:
            pl.semaphore_wait(ready.at[1], R - 1)
        spread(step, dk, dk_ssem, dk_rsem)
        if step == 0:
            launch(sides)
        else:
            pl.when(side == 1)(lambda: launch(sides[1:] + sides[:1]))

    def solve(step):
        total = unpacked(gathered_sum(step, pk, pk_ssem, pk_rsem, jnp.zeros(pk.shape[2:], F32)))
        solved = lax.dot_general(
            total, cinv_p[...], (((1,), (0,)), ((), ())),
            precision=lax.Precision.HIGHEST, preferred_element_type=F32,
        )
        back = solved.astype(BF)
        gamma = pick(total, NC)
        bend = jnp.sum(total * back.astype(F32), axis=1, keepdims=True)
        return back, gamma, bend

    def bent(back, first, last):
        twice = jnp.concatenate([back, back], axis=1)
        return jnp.concatenate([dot_nn(twice, mm[q]) for q in range(first, last)], axis=1)

    def slope(step, total, bend):
        return jnp.sum(jnp.where(diag, total, 0.0), axis=1, keepdims=True) + bend

    def meet_own(step):
        for k in range(1, R):
            q = lax.rem(r + R - k, R)
            take = functools.partial(wait_slot, blocks.at[step], own_rsem.at[step, k - 1], q)
            if step == 0:
                take()
            else:
                pl.when(q < half_r)(take)

    def meet(step, d):
        for j in range(half_r):
            q = (1 - d) * half_r + j
            wait_slot(blocks.at[step], nbr_rsem.at[step, lax.rem(r - q + R, R)], R + q)

    def meeting(step, d):
        start = (1 - d) * half_r
        theirs = jnp.concatenate([blocks[step, R + start + j] for j in range(half_r)], axis=1)
        mine = jnp.concatenate([blocks[step, d * half_r + j] for j in range(half_r)], axis=1)
        return mine.astype(F32) + dot_nn(theirs, hots[d])

    split(0, z0)
    split(1, z0_r)
    local0 = acc[...] + dot_nn(z0_r.astype(BF), turned[1])
    product(0, local0, r0, z0)

    hot_next = hot_ids(nxt)
    hot_prev = hot_ids(prv)
    for k in range(R):
        wait_slot(cmn, cmn_rsem.at[k], lax.rem(r + R - k, R))
    for q in range(R):
        mm[q, W : 2 * W] = spreadout(hot_next if q < half_r else hot_prev, cmn[q]).astype(BF)
    right = dot_nn(jnp.concatenate([mm[q, W : 2 * W] for q in range(half_r)], axis=1), hots[1]).astype(BF)
    left = dot_nn(jnp.concatenate([mm[q, W : 2 * W] for q in range(half_r, R)], axis=1), hots[0]).astype(BF)
    for q in range(R):
        at = (q % half_r) * B
        mm[q, W : 2 * W] = (left if q < half_r else right)[:, at : at + B]

    early = jnp.where(s == 0, 1, 0)
    late = 1 - early
    meet_own(0)
    meet(0, early)
    met[early] = meeting(0, early)
    back0, gamma0, bend0 = solve(0)
    fixed[0] = bent(back0, 0, half_r)
    fixed[1] = bent(back0, half_r, R)
    steep0 = gathered_sum(0, dk, dk_ssem, dk_rsem, jnp.zeros((1, 128), F32))
    delta0 = slope(0, steep0, bend0)
    alpha0 = gamma0 / delta0

    def advance(d):
        met[d] = (met[d] + fixed[d]) * live[d]
        z = zz[d] - alpha0 * (wt[d] * met[d])
        split(d, z)
        return z.astype(BF)

    acc[...] = dot_nn(advance(early), turned[early])
    meet(0, late)
    met[late] = meeting(0, late)
    last = advance(late)
    wl0 = met[0]
    r1 = r0 - alpha0 * wl0
    z1 = jnp.concatenate([zs[q] for q in range(half_r)], axis=1)
    local1 = acc[...] + dot_nn(last, turned[late])
    product(1, local1, r1, z1)
    back1, gamma1, bend1 = solve(1)
    fix = bent(back1, 0, half_r)
    beta = gamma1 / gamma0
    steep1 = gathered_sum(1, dk, dk_ssem, dk_rsem, jnp.zeros((1, 128), F32))
    delta1 = slope(1, steep1, bend1)
    alpha1 = gamma1 / (delta1 - beta * gamma1 / alpha0)
    sol[...] = alpha0 * z0 + alpha1 * (z1 + beta * z0)
    part = r1 - (alpha1 * beta) * wl0
    meet_own(1)
    meet(1, 0)
    res[...] = part - alpha1 * ((meeting(1, 0) + fix) * live[0])

    z_copy.wait_send()
    w_copy.wait_send()
    for copy in cm_sides + cm_rows:
        copy.wait_send()
    for step in range(2):
        def sent(count):
            gone = blocks.at[step, pl.ds(0, count)]
            remote(gone, gone, blk_ssem.at[step], blk_ssem.at[step], {"sub": nxt}).wait_send()

        if step == 0:
            sent(2 * R - 1)
        else:
            pl.when(side == 0)(functools.partial(sent, R - 1))
            pl.when(side == 1)(functools.partial(sent, R))
        for store, ssem, rsem in ((pk, pk_ssem, pk_rsem), (dk, dk_ssem, dk_rsem)):
            rest = store.at[step, pl.ds(0, store.shape[1] - 1)]
            remote(rest, rest, ssem.at[step], rsem.at[step], {"sub": nxt}).wait_send()


def finish(a, b, x, y, sem):
    first = pltpu.make_async_copy(a, x.at[0], sem.at[0])
    second = pltpu.make_async_copy(b, y.at[0], sem.at[1])
    first.start()
    second.start()
    first.wait()
    second.wait()


def per_device(S, R, loads, weights, dual_ops, corner_maps, coarse_inverse, corner_ids,
               iface_sizes, left_partner, right_partner):
    _, C, H = loads.shape
    _, B, full = dual_ops.shape
    J = corner_maps.shape[1]
    NC = coarse_inverse.shape[0]
    W = (NC + 1 + 127) // 128 * 128
    G = S * R
    fold = (16 * (J // 16), B + B // 2) if J % 16 == 8 and J < 32 else (J, B)
    DMA = pltpu.SemaphoreType.DMA
    hbm = pl.BlockSpec(memory_space=pltpu.HBM)
    vmem = pl.BlockSpec(memory_space=pltpu.VMEM)
    given = [
        pltpu.with_memory_space_constraint(x, pltpu.HBM)
        for x in (loads, weights, dual_ops, corner_maps, coarse_inverse, corner_ids, iface_sizes,
                  left_partner, right_partner)
    ]
    held = pltpu.VMEM((C, H), F32)
    made = pl.pallas_call(
        functools.partial(kernel, S, R),
        out_shape=(held, held),
        in_specs=[hbm] * 9,
        out_specs=(vmem, vmem),
        scratch_shapes=[
            pltpu.VMEM((C, H), F32), pltpu.VMEM((1, H), F32), pltpu.VMEM((B, full), BF),
            pltpu.VMEM((NC, NC), F32), pltpu.VMEM((W, W), F32), pltpu.VMEM(corner_ids.shape, jnp.int32),
            pltpu.VMEM((1, H), jnp.int32), pltpu.VMEM((1, H), jnp.int32), pltpu.SMEM(iface_sizes.shape, jnp.int32),
            pltpu.VMEM((C, H), BF), pltpu.VMEM((C, H), BF), pltpu.VMEM((1, H), F32),
            pltpu.VMEM((J, B), BF), pltpu.VMEM((R,) + fold, BF), pltpu.VMEM((R,) + fold, BF),
            pltpu.VMEM((R, 2 * W, B), BF),
            pltpu.VMEM((2, H, H), BF), pltpu.VMEM((R, C, B), F32), pltpu.VMEM((C, B), F32),
            pltpu.VMEM((2, H, B), BF), pltpu.VMEM((2, C, H), F32), pltpu.VMEM((2, 1, H), F32), pltpu.VMEM((2, 1, H), F32),
            pltpu.VMEM((2, C, H), F32), pltpu.VMEM((2, C, H), F32),
            pltpu.VMEM((2, 2 * R, C, B), BF), pltpu.VMEM((2, S, 8 if C == 16 and W == 128 and NC < 64 else C, W), F32),
            pltpu.VMEM((2, G, 1, 128), F32),
            DMA((8,)), DMA, DMA((4,)), DMA((R - 1,)), DMA((R - 1,)), DMA((R,)), DMA((R,)),
            DMA((2,)), DMA((2, R - 1)), DMA((2, R)), DMA((2,)), DMA((2,)), DMA((2,)), DMA((2,)), pltpu.SemaphoreType.REGULAR((2,)),
        ],
        compiler_params=pltpu.CompilerParams(
            collective_id=0, has_side_effects=True, vmem_limit_bytes=LIMIT
        ),
    )(*given)
    done = jax.ShapeDtypeStruct((1, C, H), F32)
    return pl.pallas_call(
        finish,
        out_shape=(done, done),
        in_specs=[vmem] * 2,
        out_specs=(hbm, hbm),
        scratch_shapes=[DMA((2,))],
        compiler_params=pltpu.CompilerParams(vmem_limit_bytes=2**20),
    )(*[pltpu.with_memory_space_constraint(x, pltpu.VMEM) for x in made])


def solution(mesh):
    placed = (
        P(("parts", "sub"), "col", None),
        P(("parts", "sub"), None),
        P(("parts", "sub"), "row", None),
        P(("parts", "sub"), None, "row"),
        P("parts", None),
        P("parts", None),
        P("parts"),
        P(("parts", "sub"), None),
        P(("parts", "sub"), None),
    )
    return jax.shard_map(
        functools.partial(per_device, mesh.shape["sub"], mesh.shape["row"]),
        mesh=mesh,
        in_specs=placed,
        out_specs=(P(("parts", "sub"), "col", None), P(("parts", "sub"), "col", None)),
        check_vma=False,
    )
```

```python
import functools

import jax
import jax.numpy as jnp
from jax import lax
from jax.experimental import pallas as pl
from jax.experimental.pallas import tpu as pltpu
from jax.sharding import PartitionSpec as P

MESH = pl.DeviceIdType.MESH
LIMIT = 40 * 2**20
BF = jnp.bfloat16
F32 = jnp.float32


def each(count, body):
    if count <= 8:
        for at in range(count):
            body(at)
    else:
        lax.fori_loop(0, count, lambda at, _: (body(at), 0)[1], 0)


def dot_nt(a, b):
    return lax.dot_general(a, b, (((1,), (1,)), ((), ())), preferred_element_type=F32)


def dot_nn(a, b):
    return lax.dot_general(a, b, (((1,), (0,)), ((), ())), preferred_element_type=F32)


def kernel(
    S, R, loads, weights, op, cm, cinv, ids, sizes, lmap, rmap, sol, res,
    loads_v, w_v, op_v, cv, cinv_p, ids_v, lmap_v, rmap_v, sizes_v,
    zsend, zrecv, wrecv, cm_v, cmo, cmn, mm, hots, zs, acc, turned, zz, wt, live, fixed, met,
    blocks, pk, dk,
    in_sem, op_sem, z_sem, cmo_ssem, cmo_rsem, cmn_ssem, cmn_rsem,
    blk_ssem, own_rsem, nbr_rsem, pk_ssem, pk_rsem, dk_ssem, dk_rsem, ready,
):
    s = lax.axis_index("sub")
    r = lax.axis_index("row")
    G = S * R
    me = s * R + r
    C, H = loads_v.shape
    B = op_v.shape[0]
    NC = cv.shape[0]
    W = cinv_p.shape[1]
    half_r = R // 2
    nxt = lax.rem(s + 1, S)
    prv = lax.rem(s + S - 1, S)
    side = r // half_r
    toward = lax.rem(s + S - 1 + 2 * side, S)

    barrier = pltpu.get_barrier_semaphore()

    def peer(k):
        g = lax.rem(me + k + 1, G)
        return g, {"sub": g // R, "row": lax.rem(g, R)}

    def greet(k):
        _, who = peer(k)
        pl.semaphore_signal(barrier, inc=1, device_id=who, device_id_type=MESH)

    def tell(semaphore, k):
        pl.semaphore_signal(
            semaphore, inc=1, device_id={"row": lax.rem(r + k, R)}, device_id_type=MESH
        )

    close = S <= 4
    if close:
        for other in (nxt, prv) if S > 2 else (nxt,):
            pl.semaphore_signal(barrier, inc=1, device_id={"sub": other}, device_id_type=MESH)
        for k in range(1, R):
            tell(barrier, k)
        met_first = (2 if S > 2 else 1) + R - 1
    else:
        each(G - 1, greet)
        met_first = G - 1

    ins = [
        pltpu.make_async_copy(src, dst, in_sem.at[i])
        for i, (src, dst) in enumerate([
            (loads.at[0], loads_v), (weights, w_v), (sizes, sizes_v), (rmap, rmap_v), (lmap, lmap_v),
            (ids, ids_v), (cinv, cv), (cm.at[0], cm_v),
        ])
    ]
    for copy in ins:
        copy.start()
    op_copy = pltpu.make_async_copy(op.at[0], op_v, op_sem)
    op_copy.start()

    for copy in ins[:3]:
        copy.wait()
    lanes = lax.broadcasted_iota(jnp.int32, (1, H), 1)
    live_l = (lanes < sizes_v[prv]).astype(F32)
    live[0] = live_l
    size_after = sizes_v[s]
    w_l = w_v[...]
    r0 = loads_v[...] * live_l
    z0 = w_l * r0
    zsend[...] = z0.astype(BF)
    zz[0] = z0
    wt[0] = w_l

    ins[7].wait()
    J = cm_v.shape[0]
    J0 = cmo.shape[1]
    own_map = cm_v[...].astype(F32)
    if J0 < J:
        tail = own_map[J0:]
        folded = jnp.concatenate([tail[:, : B // 2], tail[:, B // 2 :]], axis=0)
        cmo[r] = jnp.concatenate([own_map[:J0], folded], axis=1).astype(BF)
    else:
        cmo[r] = own_map.astype(BF)

    def spreadout(hot, kept):
        if J0 == J:
            return dot_nn(hot, kept)
        tail = kept[:, B:].astype(F32)
        lower = jnp.concatenate([tail[: J - J0], tail[J - J0 :]], axis=1)
        return dot_nn(hot, jnp.concatenate([kept[:, :B].astype(F32), lower], axis=0).astype(BF))

    pl.semaphore_wait(barrier, met_first)

    def remote(src, dst, ssem, rsem, who):
        return pltpu.make_async_remote_copy(
            src_ref=src, dst_ref=dst, send_sem=ssem, recv_sem=rsem, device_id=who, device_id_type=MESH
        )

    z_copy = remote(zsend, zrecv, z_sem.at[0], z_sem.at[1], {"sub": prv})
    w_copy = remote(w_v, wrecv, z_sem.at[2], z_sem.at[3], {"sub": prv})
    z_copy.start()
    w_copy.start()
    for k in range(1, R):
        tell(ready.at[0], k)

    def to_row(src, dst, ssem, rsem, k):
        return remote(src, dst.at[r], ssem, rsem, {"row": lax.rem(r + k, R)})

    def to_side(src, dst, ssem, rsem, k):
        return remote(src, dst.at[r], ssem, rsem, {"sub": toward, "row": lax.rem(r + k, R)})

    def wait_slot(dst, rsem, q):
        remote(dst.at[q], dst.at[q], rsem, rsem, {"sub": nxt}).wait_recv()

    cm_sides = [to_side(cmo.at[r], cmn, cmn_ssem.at[k], cmn_rsem.at[k], k) for k in range(R)]
    cm_rows = [to_row(cmo.at[r], cmo, cmo_ssem.at[k - 1], cmo_rsem.at[k - 1], k) for k in range(1, R)]
    def launch(copies):
        for copy in copies:
            copy.start()

    far = jnp.logical_or(s == 0, s == S - 1)
    launch(cm_sides[:1])
    launch(cm_rows)

    ins[3].wait()
    ins[4].wait()
    right_map = rmap_v[...]
    left_map = lmap_v[...]
    live[1] = (right_map < size_after).astype(F32)

    def hot(target, the_map):
        step = 128
        for c in range(H // step):
            rows = lax.broadcasted_iota(jnp.int32, (step, H), 0) + c * step
            target[pl.ds(c * step, step), :] = (rows == the_map).astype(F32).astype(BF)

    hot(hots.at[1], right_map)
    hot(hots.at[0], left_map)
    ins[5].wait()
    ins[6].wait()
    c_hi = cv[...].astype(BF).astype(F32)
    cinv_p[...] = jnp.zeros_like(cinv_p)
    cinv_p[0:NC, 0:NC] = c_hi
    cinv_p[W : W + NC, 0:NC] = c_hi
    cinv_p[2 * W : 2 * W + NC, 0:NC] = cv[...] - c_hi

    pl.semaphore_wait(ready.at[0], R - 1)
    pl.when(far)(lambda: launch(cm_sides[1:]))

    def hot_ids(t):
        row = ids_v[pl.ds(t, 1), :]
        rows = lax.broadcasted_iota(jnp.int32, (W, row.shape[1]), 0)
        return (rows == row).astype(F32).astype(BF)

    hot_own = hot_ids(s)
    mm[r, 0:W] = spreadout(hot_own, cmo[r]).astype(BF)

    op_copy.wait()
    step = 256
    for c in range(2 * H // step):
        turned[c * step // H, c * step % H : c * step % H + step, :] = op_v[:, c * step : (c + 1) * step].T
    acc[...] = dot_nn(z0.astype(BF), turned[0])

    for k in range(1, R):
        q = lax.rem(r + R - k, R)
        wait_slot(cmo, cmo_rsem.at[k - 1], q)
        mm[q, 0:W] = spreadout(hot_own, cmo[q]).astype(BF)
    pl.when(jnp.logical_not(far))(lambda: launch(cm_sides[1:]))
    z_copy.wait_recv()
    w_copy.wait_recv()
    for k in range(1, R):
        tell(ready.at[1], k)
    z0_r = dot_nn(zrecv[...], hots[1])
    zz[1] = z0_r

    col = lax.broadcasted_iota(jnp.int32, (C, W), 1)
    cold = lax.broadcasted_iota(jnp.int32, (C, 128), 1)
    diag = cold == lax.broadcasted_iota(jnp.int32, (C, 128), 0)

    def pick(value, lane):
        return jnp.sum(jnp.where(col == lane, value, 0.0), axis=1, keepdims=True)

    fold = C == 16 and W == 128 and NC < 64

    def packed(value):
        return value[:8] + pltpu.roll(value[8:], 64, 1) if fold else value

    def unpacked(value):
        if not fold:
            return value
        low = lax.broadcasted_iota(jnp.int32, value.shape, 1) < 64
        return jnp.concatenate(
            [jnp.where(low, value, 0.0), pltpu.roll(jnp.where(low, 0.0, value), 64, 1)], axis=0
        )

    def spread(step, store, ssem, rsem):
        count = store.shape[1]
        slot = me if count == G else s

        def one(k):
            who = peer(k)[1] if count == G else {"sub": lax.rem(s + k + 1, S)}
            remote(store.at[step, slot], store.at[step, slot], ssem.at[step], rsem.at[step], who).start()

        each(count - 1, one)

    def gathered_sum(step, store, ssem, rsem, zero):
        count = store.shape[1]
        rest = store.at[step, pl.ds(0, count - 1)]
        remote(rest, rest, ssem.at[step], rsem.at[step], {"sub": nxt}).wait_recv()
        if count <= 8:
            total = store[step, 0]
            for g in range(1, count):
                total = total + store[step, g]
            return total
        return lax.fori_loop(0, count, lambda g, t: t + store[step, g], zero)

    def split(d, z):
        for j in range(half_r):
            zs[d * half_r + j] = z[:, j * B : (j + 1) * B]

    def product(step, local, r_left, z_left):
        blocks[step, r] = local.astype(BF)
        mine = blocks.at[step, r]
        delta = jnp.sum(zs[r] * local, axis=1, keepdims=True)
        dk[step, me] = jnp.sum(jnp.where(diag, delta, 0.0), axis=0, keepdims=True)
        gamma = jnp.sum(r_left * z_left, axis=1, keepdims=True)
        corner = jnp.where(col == NC, gamma, 0.0)
        for q in range(R):
            corner = corner + dot_nt(zs[q].astype(BF), mm[q, 0:W])
        pk[step, s] = packed(corner)
        nbr = blocks.at[step, pl.ds(R, R)]
        sides = [to_side(mine, nbr, blk_ssem.at[step], nbr_rsem.at[step, k], k) for k in range(R)]
        rows = [to_row(mine, blocks.at[step], blk_ssem.at[step], own_rsem.at[step, k - 1], k) for k in range(1, R)]

        if step == 0:
            spread(step, pk, pk_ssem, pk_rsem)
            launch(rows)
            pl.semaphore_wait(ready.at[1], R - 1)
            spread(step, dk, dk_ssem, dk_rsem)
            launch(sides)
        else:
            spread(step, pk, pk_ssem, pk_rsem)
            pl.when(side == 0)(lambda: launch(rows))
            spread(step, dk, dk_ssem, dk_rsem)
            pl.when(side == 1)(lambda: launch(sides[1:] + sides[:1]))

    def solve(step):
        total = unpacked(gathered_sum(step, pk, pk_ssem, pk_rsem, jnp.zeros(pk.shape[2:], F32)))
        t_hi = total.astype(BF)
        t_lo = (total - t_hi.astype(F32)).astype(BF)
        solved = dot_nn(jnp.concatenate([t_hi, t_lo, t_hi], axis=1), cinv_p[...].astype(BF))
        back = solved.astype(BF)
        gamma = pick(total, NC)
        bend = jnp.sum(total * back.astype(F32), axis=1, keepdims=True)
        return back, gamma, bend

    def bent(back, first, last):
        twice = jnp.concatenate([back, back], axis=1)
        return jnp.concatenate([dot_nn(twice, mm[q]) for q in range(first, last)], axis=1)

    def slope(step, total, bend):
        return jnp.sum(jnp.where(diag, total, 0.0), axis=1, keepdims=True) + bend

    def meet_own(step):
        for k in range(1, R):
            q = lax.rem(r + R - k, R)
            take = functools.partial(wait_slot, blocks.at[step], own_rsem.at[step, k - 1], q)
            if step == 0:
                take()
            else:
                pl.when(q < half_r)(take)

    def meet(step, d):
        for j in range(half_r):
            q = (1 - d) * half_r + j
            wait_slot(blocks.at[step], nbr_rsem.at[step, lax.rem(r - q + R, R)], R + q)

    def meeting(step, d):
        start = (1 - d) * half_r
        theirs = jnp.concatenate([blocks[step, R + start + j] for j in range(half_r)], axis=1)
        mine = jnp.concatenate([blocks[step, d * half_r + j] for j in range(half_r)], axis=1)
        return mine.astype(F32) + dot_nn(theirs, hots[d])

    split(0, z0)
    split(1, z0_r)
    local0 = acc[...] + dot_nn(z0_r.astype(BF), turned[1])
    product(0, local0, r0, z0)

    w_in = wrecv[...]
    w_hi = w_in.astype(BF)
    w_lo = (w_in - w_hi.astype(F32)).astype(BF)
    pad = lax.broadcasted_iota(jnp.int32, (16, H), 0)
    w_rows = jnp.where(pad == 0, w_hi.astype(F32), jnp.where(pad == 1, w_lo.astype(F32), 0.0))
    w_turned = dot_nn(w_rows.astype(BF), hots[1])
    wt[1] = w_turned[0:1] + w_turned[1:2]
    hot_next = hot_ids(nxt)
    hot_prev = hot_ids(prv)
    for k in range(R):
        wait_slot(cmn, cmn_rsem.at[k], lax.rem(r + R - k, R))
    for q in range(R):
        mm[q, W : 2 * W] = spreadout(hot_next if q < half_r else hot_prev, cmn[q]).astype(BF)
    right = dot_nn(jnp.concatenate([mm[q, W : 2 * W] for q in range(half_r)], axis=1), hots[1]).astype(BF)
    left = dot_nn(jnp.concatenate([mm[q, W : 2 * W] for q in range(half_r, R)], axis=1), hots[0]).astype(BF)
    for q in range(R):
        at = (q % half_r) * B
        mm[q, W : 2 * W] = (left if q < half_r else right)[:, at : at + B]

    early = jnp.where(s == 0, 1, 0)
    late = 1 - early
    meet_own(0)
    meet(0, early)
    met[early] = meeting(0, early)
    back0, gamma0, bend0 = solve(0)
    fixed[0] = bent(back0, 0, half_r)
    fixed[1] = bent(back0, half_r, R)
    steep0 = gathered_sum(0, dk, dk_ssem, dk_rsem, jnp.zeros((1, 128), F32))
    delta0 = slope(0, steep0, bend0)
    alpha0 = gamma0 / delta0

    def advance(d):
        met[d] = (met[d] + fixed[d]) * live[d]
        z = zz[d] - alpha0 * (wt[d] * met[d])
        split(d, z)
        return z.astype(BF)

    acc[...] = dot_nn(advance(early), turned[early])
    meet(0, late)
    met[late] = meeting(0, late)
    last = advance(late)
    wl0 = met[0]
    r1 = r0 - alpha0 * wl0
    z1 = jnp.concatenate([zs[q] for q in range(half_r)], axis=1)
    local1 = acc[...] + dot_nn(last, turned[late])
    product(1, local1, r1, z1)
    back1, gamma1, bend1 = solve(1)
    fix = bent(back1, 0, half_r)
    beta = gamma1 / gamma0
    steep1 = gathered_sum(1, dk, dk_ssem, dk_rsem, jnp.zeros((1, 128), F32))
    delta1 = slope(1, steep1, bend1)
    alpha1 = gamma1 / (delta1 - beta * gamma1 / alpha0)
    sol[...] = alpha0 * z0 + alpha1 * (z1 + beta * z0)
    part = r1 - (alpha1 * beta) * wl0
    meet_own(1)
    meet(1, 0)
    res[...] = part - alpha1 * ((meeting(1, 0) + fix) * live[0])

    z_copy.wait_send()
    w_copy.wait_send()
    for copy in cm_sides + cm_rows:
        copy.wait_send()
    for step in range(2):
        def sent(count):
            gone = blocks.at[step, pl.ds(0, count)]
            remote(gone, gone, blk_ssem.at[step], blk_ssem.at[step], {"sub": nxt}).wait_send()

        if step == 0:
            sent(2 * R - 1)
        else:
            pl.when(side == 0)(functools.partial(sent, R - 1))
            pl.when(side == 1)(functools.partial(sent, R))
        for store, ssem, rsem in ((pk, pk_ssem, pk_rsem), (dk, dk_ssem, dk_rsem)):
            rest = store.at[step, pl.ds(0, store.shape[1] - 1)]
            remote(rest, rest, ssem.at[step], rsem.at[step], {"sub": nxt}).wait_send()


def finish(a, b, x, y, sem):
    first = pltpu.make_async_copy(a, x.at[0], sem.at[0])
    second = pltpu.make_async_copy(b, y.at[0], sem.at[1])
    first.start()
    second.start()
    first.wait()
    second.wait()


def per_device(S, R, loads, weights, dual_ops, corner_maps, coarse_inverse, corner_ids,
               iface_sizes, left_partner, right_partner):
    _, C, H = loads.shape
    _, B, full = dual_ops.shape
    J = corner_maps.shape[1]
    NC = coarse_inverse.shape[0]
    W = (NC + 1 + 127) // 128 * 128
    G = S * R
    fold = (16 * (J // 16), B + B // 2) if J % 16 == 8 and J < 32 else (J, B)
    DMA = pltpu.SemaphoreType.DMA
    hbm = pl.BlockSpec(memory_space=pltpu.HBM)
    vmem = pl.BlockSpec(memory_space=pltpu.VMEM)
    given = [
        pltpu.with_memory_space_constraint(x, pltpu.HBM)
        for x in (loads, weights, dual_ops, corner_maps, coarse_inverse, corner_ids, iface_sizes,
                  left_partner, right_partner)
    ]
    held = pltpu.VMEM((C, H), F32)
    made = pl.pallas_call(
        functools.partial(kernel, S, R),
        out_shape=(held, held),
        in_specs=[hbm] * 9,
        out_specs=(vmem, vmem),
        scratch_shapes=[
            pltpu.VMEM((C, H), F32), pltpu.VMEM((1, H), F32), pltpu.VMEM((B, full), BF),
            pltpu.VMEM((NC, NC), F32), pltpu.VMEM((3 * W, W), F32), pltpu.VMEM(corner_ids.shape, jnp.int32),
            pltpu.VMEM((1, H), jnp.int32), pltpu.VMEM((1, H), jnp.int32), pltpu.SMEM(iface_sizes.shape, jnp.int32),
            pltpu.VMEM((C, H), BF), pltpu.VMEM((C, H), BF), pltpu.VMEM((1, H), F32),
            pltpu.VMEM((J, B), BF), pltpu.VMEM((R,) + fold, BF), pltpu.VMEM((R,) + fold, BF),
            pltpu.VMEM((R, 2 * W, B), BF),
            pltpu.VMEM((2, H, H), BF), pltpu.VMEM((R, C, B), F32), pltpu.VMEM((C, B), F32),
            pltpu.VMEM((2, H, B), BF), pltpu.VMEM((2, C, H), F32), pltpu.VMEM((2, 1, H), F32), pltpu.VMEM((2, 1, H), F32),
            pltpu.VMEM((2, C, H), F32), pltpu.VMEM((2, C, H), F32),
            pltpu.VMEM((2, 2 * R, C, B), BF), pltpu.VMEM((2, S, 8 if C == 16 and W == 128 and NC < 64 else C, W), F32),
            pltpu.VMEM((2, G, 1, 128), F32),
            DMA((8,)), DMA, DMA((4,)), DMA((R - 1,)), DMA((R - 1,)), DMA((R,)), DMA((R,)),
            DMA((2,)), DMA((2, R - 1)), DMA((2, R)), DMA((2,)), DMA((2,)), DMA((2,)), DMA((2,)), pltpu.SemaphoreType.REGULAR((2,)),
        ],
        compiler_params=pltpu.CompilerParams(
            collective_id=0, has_side_effects=True, vmem_limit_bytes=LIMIT
        ),
    )(*given)
    done = jax.ShapeDtypeStruct((1, C, H), F32)
    return pl.pallas_call(
        finish,
        out_shape=(done, done),
        in_specs=[vmem] * 2,
        out_specs=(hbm, hbm),
        scratch_shapes=[DMA((2,))],
        compiler_params=pltpu.CompilerParams(vmem_limit_bytes=2**20),
    )(*[pltpu.with_memory_space_constraint(x, pltpu.VMEM) for x in made])


def solution(mesh):
    placed = (
        P(("parts", "sub"), "col", None),
        P(("parts", "sub"), None),
        P(("parts", "sub"), "row", None),
        P(("parts", "sub"), None, "row"),
        P("parts", None),
        P("parts", None),
        P("parts"),
        P(("parts", "sub"), None),
        P(("parts", "sub"), None),
    )
    return jax.shard_map(
        functools.partial(per_device, mesh.shape["sub"], mesh.shape["row"]),
        mesh=mesh,
        in_specs=placed,
        out_specs=(P(("parts", "sub"), "col", None), P(("parts", "sub"), "col", None)),
        check_vma=False,
    )
```

```python
import functools

import jax
import jax.numpy as jnp
from jax import lax
from jax.experimental import pallas as pl
from jax.experimental.pallas import tpu as pltpu
from jax.sharding import PartitionSpec as P

MESH = pl.DeviceIdType.MESH
LIMIT = 40 * 2**20
BF = jnp.bfloat16
F32 = jnp.float32


def each(count, body):
    if count <= 8:
        for at in range(count):
            body(at)
    else:
        lax.fori_loop(0, count, lambda at, _: (body(at), 0)[1], 0)


def dot_nt(a, b):
    return lax.dot_general(a, b, (((1,), (1,)), ((), ())), preferred_element_type=F32)


def dot_nn(a, b):
    return lax.dot_general(a, b, (((1,), (0,)), ((), ())), preferred_element_type=F32)


def kernel(
    S, R, loads, weights, op, cm, cinv, ids, sizes, lmap, rmap, sol, res,
    loads_v, w_v, op_v, cv, cinv_p, ids_v, lmap_v, rmap_v, sizes_v,
    zsend, zrecv, wrecv, cm_v, cmo, cmn, mm, hots, zs, acc, turned, zz, wt, live, fixed, met,
    blocks, pk, dk,
    in_sem, op_sem, z_sem, cmo_ssem, cmo_rsem, cmn_ssem, cmn_rsem,
    blk_ssem, own_rsem, nbr_rsem, pk_ssem, pk_rsem, dk_ssem, dk_rsem, ready,
):
    s = lax.axis_index("sub")
    r = lax.axis_index("row")
    G = S * R
    me = s * R + r
    C, H = loads_v.shape
    B = op_v.shape[0]
    NC = cv.shape[0]
    W = cinv_p.shape[1]
    half_r = R // 2
    nxt = lax.rem(s + 1, S)
    prv = lax.rem(s + S - 1, S)
    side = r // half_r
    toward = lax.rem(s + S - 1 + 2 * side, S)

    barrier = pltpu.get_barrier_semaphore()

    def peer(k):
        g = lax.rem(me + k + 1, G)
        return g, {"sub": g // R, "row": lax.rem(g, R)}

    def greet(k):
        _, who = peer(k)
        pl.semaphore_signal(barrier, inc=1, device_id=who, device_id_type=MESH)

    def tell(semaphore, k):
        pl.semaphore_signal(
            semaphore, inc=1, device_id={"row": lax.rem(r + k, R)}, device_id_type=MESH
        )

    close = S <= 4
    if close:
        for other in (nxt, prv) if S > 2 else (nxt,):
            pl.semaphore_signal(barrier, inc=1, device_id={"sub": other}, device_id_type=MESH)
        for k in range(1, R):
            tell(barrier, k)
        met_first = (2 if S > 2 else 1) + R - 1
    else:
        each(G - 1, greet)
        met_first = G - 1

    ins = [
        pltpu.make_async_copy(src, dst, in_sem.at[i])
        for i, (src, dst) in enumerate([
            (loads.at[0], loads_v), (weights, w_v), (sizes, sizes_v), (rmap, rmap_v), (lmap, lmap_v),
            (ids, ids_v), (cinv, cv), (cm.at[0], cm_v),
        ])
    ]
    for copy in ins:
        copy.start()
    op_copy = pltpu.make_async_copy(op.at[0], op_v, op_sem)
    op_copy.start()

    for copy in ins[:3]:
        copy.wait()
    lanes = lax.broadcasted_iota(jnp.int32, (1, H), 1)
    live_l = (lanes < sizes_v[prv]).astype(F32)
    live[0] = live_l
    size_after = sizes_v[s]
    w_l = w_v[...]
    r0 = loads_v[...] * live_l
    z0 = w_l * r0
    zsend[...] = z0.astype(BF)
    zz[0] = z0
    wt[0] = w_l

    ins[7].wait()
    J = cm_v.shape[0]
    J0 = cmo.shape[1]
    own_map = cm_v[...].astype(F32)
    if J0 < J:
        tail = own_map[J0:]
        folded = jnp.concatenate([tail[:, : B // 2], tail[:, B // 2 :]], axis=0)
        cmo[r] = jnp.concatenate([own_map[:J0], folded], axis=1).astype(BF)
    else:
        cmo[r] = own_map.astype(BF)

    def spreadout(hot, kept):
        if J0 == J:
            return dot_nn(hot, kept)
        tail = kept[:, B:].astype(F32)
        lower = jnp.concatenate([tail[: J - J0], tail[J - J0 :]], axis=1)
        return dot_nn(hot, jnp.concatenate([kept[:, :B].astype(F32), lower], axis=0).astype(BF))

    pl.semaphore_wait(barrier, met_first)

    def remote(src, dst, ssem, rsem, who):
        return pltpu.make_async_remote_copy(
            src_ref=src, dst_ref=dst, send_sem=ssem, recv_sem=rsem, device_id=who, device_id_type=MESH
        )

    z_copy = remote(zsend, zrecv, z_sem.at[0], z_sem.at[1], {"sub": prv})
    w_copy = remote(w_v, wrecv, z_sem.at[2], z_sem.at[3], {"sub": prv})
    z_copy.start()
    w_copy.start()
    for k in range(1, R):
        tell(ready.at[0], k)

    def to_row(src, dst, ssem, rsem, k):
        return remote(src, dst.at[r], ssem, rsem, {"row": lax.rem(r + k, R)})

    def to_side(src, dst, ssem, rsem, k):
        return remote(src, dst.at[r], ssem, rsem, {"sub": toward, "row": lax.rem(r + k, R)})

    def wait_slot(dst, rsem, q):
        remote(dst.at[q], dst.at[q], rsem, rsem, {"sub": nxt}).wait_recv()

    cm_sides = [to_side(cmo.at[r], cmn, cmn_ssem.at[k], cmn_rsem.at[k], k) for k in range(R)]
    cm_rows = [to_row(cmo.at[r], cmo, cmo_ssem.at[k - 1], cmo_rsem.at[k - 1], k) for k in range(1, R)]
    def launch(copies):
        for copy in copies:
            copy.start()

    far = jnp.logical_or(s == 0, s == S - 1)
    launch(cm_sides[:1])
    launch(cm_rows)

    ins[3].wait()
    ins[4].wait()
    right_map = rmap_v[...]
    left_map = lmap_v[...]
    live[1] = (right_map < size_after).astype(F32)

    def hot(target, the_map):
        step = 128
        for c in range(H // step):
            rows = lax.broadcasted_iota(jnp.int32, (step, H), 0) + c * step
            target[pl.ds(c * step, step), :] = (rows == the_map).astype(F32).astype(BF)

    hot(hots.at[1], right_map)
    hot(hots.at[0], left_map)
    ins[5].wait()
    ins[6].wait()
    c_hi = cv[...].astype(BF).astype(F32)
    cinv_p[...] = jnp.zeros_like(cinv_p)
    cinv_p[0:NC, 0:NC] = c_hi
    cinv_p[W : W + NC, 0:NC] = c_hi
    cinv_p[2 * W : 2 * W + NC, 0:NC] = cv[...] - c_hi

    pl.semaphore_wait(ready.at[0], R - 1)
    pl.when(far)(lambda: launch(cm_sides[1:]))

    def hot_ids(t):
        row = ids_v[pl.ds(t, 1), :]
        rows = lax.broadcasted_iota(jnp.int32, (W, row.shape[1]), 0)
        return (rows == row).astype(F32).astype(BF)

    hot_own = hot_ids(s)
    mm[r, 0:W] = spreadout(hot_own, cmo[r]).astype(BF)

    op_copy.wait()
    step = 256
    for c in range(2 * H // step):
        turned[c * step // H, c * step % H : c * step % H + step, :] = op_v[:, c * step : (c + 1) * step].T
    acc[...] = dot_nn(z0.astype(BF), turned[0])

    for k in range(1, R):
        q = lax.rem(r + R - k, R)
        wait_slot(cmo, cmo_rsem.at[k - 1], q)
        mm[q, 0:W] = spreadout(hot_own, cmo[q]).astype(BF)
    pl.when(jnp.logical_not(far))(lambda: launch(cm_sides[1:]))
    z_copy.wait_recv()
    w_copy.wait_recv()
    for k in range(1, R):
        tell(ready.at[1], k)
    z0_r = dot_nn(zrecv[...], hots[1])
    zz[1] = z0_r

    col = lax.broadcasted_iota(jnp.int32, (C, W), 1)
    cold = lax.broadcasted_iota(jnp.int32, (C, 128), 1)
    diag = cold == lax.broadcasted_iota(jnp.int32, (C, 128), 0)

    def pick(value, lane):
        return jnp.sum(jnp.where(col == lane, value, 0.0), axis=1, keepdims=True)

    fold = C == 16 and W == 128 and NC < 64

    def packed(value):
        return value[:8] + pltpu.roll(value[8:], 64, 1) if fold else value

    def unpacked(value):
        if not fold:
            return value
        low = lax.broadcasted_iota(jnp.int32, value.shape, 1) < 64
        return jnp.concatenate(
            [jnp.where(low, value, 0.0), pltpu.roll(jnp.where(low, 0.0, value), 64, 1)], axis=0
        )

    def spread(step, store, ssem, rsem):
        count = store.shape[1]
        slot = me if count == G else s

        def one(k):
            who = peer(k)[1] if count == G else {"sub": lax.rem(s + k + 1, S)}
            remote(store.at[step, slot], store.at[step, slot], ssem.at[step], rsem.at[step], who).start()

        each(count - 1, one)

    def gathered_sum(step, store, ssem, rsem, zero):
        count = store.shape[1]
        rest = store.at[step, pl.ds(0, count - 1)]
        remote(rest, rest, ssem.at[step], rsem.at[step], {"sub": nxt}).wait_recv()
        if count <= 8:
            total = store[step, 0]
            for g in range(1, count):
                total = total + store[step, g]
            return total
        return lax.fori_loop(0, count, lambda g, t: t + store[step, g], zero)

    def split(d, z):
        for j in range(half_r):
            zs[d * half_r + j] = z[:, j * B : (j + 1) * B]

    def product(step, local, r_left, z_left):
        blocks[step, r] = local.astype(BF)
        mine = blocks.at[step, r]
        delta = jnp.sum(zs[r] * local, axis=1, keepdims=True)
        dk[step, me] = jnp.sum(jnp.where(diag, delta, 0.0), axis=0, keepdims=True)
        gamma = jnp.sum(r_left * z_left, axis=1, keepdims=True)
        corner = jnp.where(col == NC, gamma, 0.0)
        for q in range(R):
            corner = corner + dot_nt(zs[q].astype(BF), mm[q, 0:W])
        pk[step, s] = packed(corner)
        nbr = blocks.at[step, pl.ds(R, R)]
        sides = [to_side(mine, nbr, blk_ssem.at[step], nbr_rsem.at[step, k], k) for k in range(R)]
        rows = [to_row(mine, blocks.at[step], blk_ssem.at[step], own_rsem.at[step, k - 1], k) for k in range(1, R)]

        def slopes(last):
            for ds in range(S):
                for dr in range(R):
                    distant = 1 < ds < S - 1 and dr > 0
                    if ds + dr > 0 and distant == last:
                        who = {"sub": lax.rem(s + ds, S), "row": lax.rem(r + dr, R)}
                        remote(dk.at[0, me], dk.at[0, me], dk_ssem.at[0], dk_rsem.at[0], who).start()

        if step == 0:
            spread(step, pk, pk_ssem, pk_rsem)
            launch(rows)
            slopes(False)
            launch(sides[1:] + sides[:1])
            pl.semaphore_wait(ready.at[1], R - 1)
            slopes(True)
        else:
            spread(step, pk, pk_ssem, pk_rsem)
            pl.when(side == 0)(lambda: launch(rows))
            spread(step, dk, dk_ssem, dk_rsem)
            pl.when(side == 1)(lambda: launch(sides[1:] + sides[:1]))

    def solve(step):
        total = unpacked(gathered_sum(step, pk, pk_ssem, pk_rsem, jnp.zeros(pk.shape[2:], F32)))
        t_hi = total.astype(BF)
        t_lo = (total - t_hi.astype(F32)).astype(BF)
        solved = dot_nn(jnp.concatenate([t_hi, t_lo, t_hi], axis=1), cinv_p[...].astype(BF))
        back = solved.astype(BF)
        gamma = pick(total, NC)
        bend = jnp.sum(total * back.astype(F32), axis=1, keepdims=True)
        return back, gamma, bend

    def bent(back, first, last):
        twice = jnp.concatenate([back, back], axis=1)
        return jnp.concatenate([dot_nn(twice, mm[q]) for q in range(first, last)], axis=1)

    def slope(step, total, bend):
        return jnp.sum(jnp.where(diag, total, 0.0), axis=1, keepdims=True) + bend

    def meet_own(step):
        for k in range(1, R):
            q = lax.rem(r + R - k, R)
            take = functools.partial(wait_slot, blocks.at[step], own_rsem.at[step, k - 1], q)
            if step == 0:
                take()
            else:
                pl.when(q < half_r)(take)

    def meet(step, d):
        for j in range(half_r):
            q = (1 - d) * half_r + j
            wait_slot(blocks.at[step], nbr_rsem.at[step, lax.rem(r - q + R, R)], R + q)

    def meeting(step, d):
        start = (1 - d) * half_r
        theirs = jnp.concatenate([blocks[step, R + start + j] for j in range(half_r)], axis=1)
        mine = jnp.concatenate([blocks[step, d * half_r + j] for j in range(half_r)], axis=1)
        return mine.astype(F32) + dot_nn(theirs, hots[d])

    split(0, z0)
    split(1, z0_r)
    local0 = acc[...] + dot_nn(z0_r.astype(BF), turned[1])
    product(0, local0, r0, z0)

    w_in = wrecv[...]
    w_hi = w_in.astype(BF)
    w_lo = (w_in - w_hi.astype(F32)).astype(BF)
    pad = lax.broadcasted_iota(jnp.int32, (16, H), 0)
    w_rows = jnp.where(pad == 0, w_hi.astype(F32), jnp.where(pad == 1, w_lo.astype(F32), 0.0))
    w_turned = dot_nn(w_rows.astype(BF), hots[1])
    wt[1] = w_turned[0:1] + w_turned[1:2]
    hot_next = hot_ids(nxt)
    hot_prev = hot_ids(prv)
    for k in range(R):
        wait_slot(cmn, cmn_rsem.at[k], lax.rem(r + R - k, R))
    for q in range(R):
        mm[q, W : 2 * W] = spreadout(hot_next if q < half_r else hot_prev, cmn[q]).astype(BF)
    right = dot_nn(jnp.concatenate([mm[q, W : 2 * W] for q in range(half_r)], axis=1), hots[1]).astype(BF)
    left = dot_nn(jnp.concatenate([mm[q, W : 2 * W] for q in range(half_r, R)], axis=1), hots[0]).astype(BF)
    for q in range(R):
        at = (q % half_r) * B
        mm[q, W : 2 * W] = (left if q < half_r else right)[:, at : at + B]

    early = jnp.where(s == 0, 1, 0)
    late = 1 - early
    meet_own(0)
    meet(0, early)
    met[early] = meeting(0, early)
    back0, gamma0, bend0 = solve(0)
    fixed[0] = bent(back0, 0, half_r)
    fixed[1] = bent(back0, half_r, R)
    steep0 = gathered_sum(0, dk, dk_ssem, dk_rsem, jnp.zeros((1, 128), F32))
    delta0 = slope(0, steep0, bend0)
    alpha0 = gamma0 / delta0

    def advance(d):
        met[d] = (met[d] + fixed[d]) * live[d]
        z = zz[d] - alpha0 * (wt[d] * met[d])
        split(d, z)
        return z.astype(BF)

    acc[...] = dot_nn(advance(early), turned[early])
    meet(0, late)
    met[late] = meeting(0, late)
    last = advance(late)
    wl0 = met[0]
    r1 = r0 - alpha0 * wl0
    z1 = jnp.concatenate([zs[q] for q in range(half_r)], axis=1)
    local1 = acc[...] + dot_nn(last, turned[late])
    product(1, local1, r1, z1)
    back1, gamma1, bend1 = solve(1)
    fix = bent(back1, 0, half_r)
    beta = gamma1 / gamma0
    steep1 = gathered_sum(1, dk, dk_ssem, dk_rsem, jnp.zeros((1, 128), F32))
    delta1 = slope(1, steep1, bend1)
    alpha1 = gamma1 / (delta1 - beta * gamma1 / alpha0)
    sol[...] = alpha0 * z0 + alpha1 * (z1 + beta * z0)
    part = r1 - (alpha1 * beta) * wl0
    meet_own(1)
    meet(1, 0)
    res[...] = part - alpha1 * ((meeting(1, 0) + fix) * live[0])

    z_copy.wait_send()
    w_copy.wait_send()
    for copy in cm_sides + cm_rows:
        copy.wait_send()
    for step in range(2):
        def sent(count):
            gone = blocks.at[step, pl.ds(0, count)]
            remote(gone, gone, blk_ssem.at[step], blk_ssem.at[step], {"sub": nxt}).wait_send()

        if step == 0:
            sent(2 * R - 1)
        else:
            pl.when(side == 0)(functools.partial(sent, R - 1))
            pl.when(side == 1)(functools.partial(sent, R))
        for store, ssem, rsem in ((pk, pk_ssem, pk_rsem), (dk, dk_ssem, dk_rsem)):
            rest = store.at[step, pl.ds(0, store.shape[1] - 1)]
            remote(rest, rest, ssem.at[step], rsem.at[step], {"sub": nxt}).wait_send()


def finish(a, b, x, y, sem):
    first = pltpu.make_async_copy(a, x.at[0], sem.at[0])
    second = pltpu.make_async_copy(b, y.at[0], sem.at[1])
    first.start()
    second.start()
    first.wait()
    second.wait()


def per_device(S, R, loads, weights, dual_ops, corner_maps, coarse_inverse, corner_ids,
               iface_sizes, left_partner, right_partner):
    _, C, H = loads.shape
    _, B, full = dual_ops.shape
    J = corner_maps.shape[1]
    NC = coarse_inverse.shape[0]
    W = (NC + 1 + 127) // 128 * 128
    G = S * R
    fold = (16 * (J // 16), B + B // 2) if J % 16 == 8 and J < 32 else (J, B)
    DMA = pltpu.SemaphoreType.DMA
    hbm = pl.BlockSpec(memory_space=pltpu.HBM)
    vmem = pl.BlockSpec(memory_space=pltpu.VMEM)
    given = [
        pltpu.with_memory_space_constraint(x, pltpu.HBM)
        for x in (loads, weights, dual_ops, corner_maps, coarse_inverse, corner_ids, iface_sizes,
                  left_partner, right_partner)
    ]
    held = pltpu.VMEM((C, H), F32)
    made = pl.pallas_call(
        functools.partial(kernel, S, R),
        out_shape=(held, held),
        in_specs=[hbm] * 9,
        out_specs=(vmem, vmem),
        scratch_shapes=[
            pltpu.VMEM((C, H), F32), pltpu.VMEM((1, H), F32), pltpu.VMEM((B, full), BF),
            pltpu.VMEM((NC, NC), F32), pltpu.VMEM((3 * W, W), F32), pltpu.VMEM(corner_ids.shape, jnp.int32),
            pltpu.VMEM((1, H), jnp.int32), pltpu.VMEM((1, H), jnp.int32), pltpu.SMEM(iface_sizes.shape, jnp.int32),
            pltpu.VMEM((C, H), BF), pltpu.VMEM((C, H), BF), pltpu.VMEM((1, H), F32),
            pltpu.VMEM((J, B), BF), pltpu.VMEM((R,) + fold, BF), pltpu.VMEM((R,) + fold, BF),
            pltpu.VMEM((R, 2 * W, B), BF),
            pltpu.VMEM((2, H, H), BF), pltpu.VMEM((R, C, B), F32), pltpu.VMEM((C, B), F32),
            pltpu.VMEM((2, H, B), BF), pltpu.VMEM((2, C, H), F32), pltpu.VMEM((2, 1, H), F32), pltpu.VMEM((2, 1, H), F32),
            pltpu.VMEM((2, C, H), F32), pltpu.VMEM((2, C, H), F32),
            pltpu.VMEM((2, 2 * R, C, B), BF), pltpu.VMEM((2, S, 8 if C == 16 and W == 128 and NC < 64 else C, W), F32),
            pltpu.VMEM((2, G, 1, 128), F32),
            DMA((8,)), DMA, DMA((4,)), DMA((R - 1,)), DMA((R - 1,)), DMA((R,)), DMA((R,)),
            DMA((2,)), DMA((2, R - 1)), DMA((2, R)), DMA((2,)), DMA((2,)), DMA((2,)), DMA((2,)), pltpu.SemaphoreType.REGULAR((2,)),
        ],
        compiler_params=pltpu.CompilerParams(
            collective_id=0, has_side_effects=True, vmem_limit_bytes=LIMIT
        ),
    )(*given)
    done = jax.ShapeDtypeStruct((1, C, H), F32)
    return pl.pallas_call(
        finish,
        out_shape=(done, done),
        in_specs=[vmem] * 2,
        out_specs=(hbm, hbm),
        scratch_shapes=[DMA((2,))],
        compiler_params=pltpu.CompilerParams(vmem_limit_bytes=2**20),
    )(*[pltpu.with_memory_space_constraint(x, pltpu.VMEM) for x in made])


def solution(mesh):
    placed = (
        P(("parts", "sub"), "col", None),
        P(("parts", "sub"), None),
        P(("parts", "sub"), "row", None),
        P(("parts", "sub"), None, "row"),
        P("parts", None),
        P("parts", None),
        P("parts"),
        P(("parts", "sub"), None),
        P(("parts", "sub"), None),
    )
    return jax.shard_map(
        functools.partial(per_device, mesh.shape["sub"], mesh.shape["row"]),
        mesh=mesh,
        in_specs=placed,
        out_specs=(P(("parts", "sub"), "col", None), P(("parts", "sub"), "col", None)),
        check_vma=False,
    )
```

```python
import functools

import jax
import jax.numpy as jnp
from jax import lax
from jax.experimental import pallas as pl
from jax.experimental.pallas import tpu as pltpu
from jax.sharding import PartitionSpec as P

MESH = pl.DeviceIdType.MESH
LIMIT = 40 * 2**20
BF = jnp.bfloat16
F32 = jnp.float32


def each(count, body):
    if count <= 8:
        for at in range(count):
            body(at)
    else:
        lax.fori_loop(0, count, lambda at, _: (body(at), 0)[1], 0)


def dot_nt(a, b):
    return lax.dot_general(a, b, (((1,), (1,)), ((), ())), preferred_element_type=F32)


def dot_nn(a, b):
    return lax.dot_general(a, b, (((1,), (0,)), ((), ())), preferred_element_type=F32)


def kernel(
    S, R, loads, weights, op, cm, cinv, ids, sizes, lmap, rmap, sol, res,
    loads_v, w_v, op_v, cv, cinv_p, ids_v, lmap_v, rmap_v, sizes_v,
    zsend, zrecv, wrecv, cm_v, cmo, cmn, mm, hots, zs, acc, turned, zz, wt, live, fixed, met,
    blocks, pk, dk,
    in_sem, op_sem, z_sem, cmo_ssem, cmo_rsem, cmn_ssem, cmn_rsem,
    blk_ssem, own_rsem, nbr_rsem, pk_ssem, pk_rsem, dk_ssem, dk_rsem, ready, led,
):
    s = lax.axis_index("sub")
    r = lax.axis_index("row")
    G = S * R
    me = s * R + r
    C, H = loads_v.shape
    B = op_v.shape[0]
    NC = cv.shape[0]
    W = cinv_p.shape[1]
    half_r = R // 2
    nxt = lax.rem(s + 1, S)
    prv = lax.rem(s + S - 1, S)
    side = r // half_r
    toward = lax.rem(s + S - 1 + 2 * side, S)

    barrier = pltpu.get_barrier_semaphore()

    def peer(k):
        g = lax.rem(me + k + 1, G)
        return g, {"sub": g // R, "row": lax.rem(g, R)}

    def greet(k):
        _, who = peer(k)
        pl.semaphore_signal(barrier, inc=1, device_id=who, device_id_type=MESH)

    def tell(semaphore, k):
        pl.semaphore_signal(
            semaphore, inc=1, device_id={"row": lax.rem(r + k, R)}, device_id_type=MESH
        )

    close = S <= 4
    if close:
        for other in (nxt, prv) if S > 2 else (nxt,):
            pl.semaphore_signal(barrier, inc=1, device_id={"sub": other}, device_id_type=MESH)
        for k in range(1, R):
            tell(barrier, k)
        met_first = (2 if S > 2 else 1) + R - 1
    else:
        each(G - 1, greet)
        met_first = G - 1

    ins = [
        pltpu.make_async_copy(src, dst, in_sem.at[i])
        for i, (src, dst) in enumerate([
            (loads.at[0], loads_v), (weights, w_v), (sizes, sizes_v), (rmap, rmap_v), (lmap, lmap_v),
            (ids, ids_v), (cinv, cv), (cm.at[0], cm_v),
        ])
    ]
    for copy in ins:
        copy.start()
    op_copy = pltpu.make_async_copy(op.at[0], op_v, op_sem)
    op_copy.start()

    for copy in ins[:3]:
        copy.wait()
    lanes = lax.broadcasted_iota(jnp.int32, (1, H), 1)
    live_l = (lanes < sizes_v[prv]).astype(F32)
    live[0] = live_l
    size_after = sizes_v[s]
    w_l = w_v[...]
    r0 = loads_v[...] * live_l
    z0 = w_l * r0
    zsend[...] = z0.astype(BF)
    zz[0] = z0
    wt[0] = w_l

    ins[7].wait()
    J = cm_v.shape[0]
    J0 = cmo.shape[1]
    own_map = cm_v[...].astype(F32)
    if J0 < J:
        tail = own_map[J0:]
        folded = jnp.concatenate([tail[:, : B // 2], tail[:, B // 2 :]], axis=0)
        cmo[r] = jnp.concatenate([own_map[:J0], folded], axis=1).astype(BF)
    else:
        cmo[r] = own_map.astype(BF)

    def spreadout(hot, kept):
        if J0 == J:
            return dot_nn(hot, kept)
        tail = kept[:, B:].astype(F32)
        lower = jnp.concatenate([tail[: J - J0], tail[J - J0 :]], axis=1)
        return dot_nn(hot, jnp.concatenate([kept[:, :B].astype(F32), lower], axis=0).astype(BF))

    pl.semaphore_wait(barrier, met_first)

    def remote(src, dst, ssem, rsem, who):
        return pltpu.make_async_remote_copy(
            src_ref=src, dst_ref=dst, send_sem=ssem, recv_sem=rsem, device_id=who, device_id_type=MESH
        )

    z_copy = remote(zsend, zrecv, z_sem.at[0], z_sem.at[1], {"sub": prv})
    w_copy = remote(w_v, wrecv, z_sem.at[2], z_sem.at[3], {"sub": prv})
    z_copy.start()
    w_copy.start()
    for k in range(1, R):
        tell(ready.at[0], k)

    def to_row(src, dst, ssem, rsem, k):
        return remote(src, dst.at[r], ssem, rsem, {"row": lax.rem(r + k, R)})

    def to_side(src, dst, ssem, rsem, k):
        return remote(src, dst.at[r], ssem, rsem, {"sub": toward, "row": lax.rem(r + k, R)})

    def wait_slot(dst, rsem, q):
        remote(dst.at[q], dst.at[q], rsem, rsem, {"sub": nxt}).wait_recv()

    cm_sides = [to_side(cmo.at[r], cmn, cmn_ssem.at[k], cmn_rsem.at[k], k) for k in range(R)]
    cm_rows = [to_row(cmo.at[r], cmo, cmo_ssem.at[k - 1], cmo_rsem.at[k - 1], k) for k in range(1, R)]
    def launch(copies):
        for copy in copies:
            copy.start()

    far = jnp.logical_or(s == 0, s == S - 1)
    launch(cm_sides[:1])
    launch(cm_rows)

    ins[3].wait()
    ins[4].wait()
    right_map = rmap_v[...]
    left_map = lmap_v[...]
    live[1] = (right_map < size_after).astype(F32)

    def hot(target, the_map):
        step = 128
        for c in range(H // step):
            rows = lax.broadcasted_iota(jnp.int32, (step, H), 0) + c * step
            target[pl.ds(c * step, step), :] = (rows == the_map).astype(F32).astype(BF)

    hot(hots.at[1], right_map)
    hot(hots.at[0], left_map)
    ins[5].wait()
    ins[6].wait()
    c_hi = cv[...].astype(BF).astype(F32)
    cinv_p[...] = jnp.zeros_like(cinv_p)
    cinv_p[0:NC, 0:NC] = c_hi
    cinv_p[W : W + NC, 0:NC] = c_hi
    cinv_p[2 * W : 2 * W + NC, 0:NC] = cv[...] - c_hi

    pl.semaphore_wait(ready.at[0], R - 1)
    pl.when(far)(lambda: launch(cm_sides[1:]))

    def hot_ids(t):
        row = ids_v[pl.ds(t, 1), :]
        rows = lax.broadcasted_iota(jnp.int32, (W, row.shape[1]), 0)
        return (rows == row).astype(F32).astype(BF)

    hot_own = hot_ids(s)
    mm[r, 0:W] = spreadout(hot_own, cmo[r]).astype(BF)

    op_copy.wait()
    step = 256
    for c in range(2 * H // step):
        turned[c * step // H, c * step % H : c * step % H + step, :] = op_v[:, c * step : (c + 1) * step].T
    acc[...] = dot_nn(z0.astype(BF), turned[0])

    for k in range(1, R):
        q = lax.rem(r + R - k, R)
        wait_slot(cmo, cmo_rsem.at[k - 1], q)
        mm[q, 0:W] = spreadout(hot_own, cmo[q]).astype(BF)
    lead = jnp.where(
        lax.broadcasted_iota(jnp.int32, (C, W), 1) == NC, jnp.sum(r0 * z0, axis=1, keepdims=True), 0.0
    )
    for q in range(half_r):
        lead = lead + dot_nt(z0[:, q * B : (q + 1) * B].astype(BF), mm[q, 0:W])
    led[...] = lead
    pl.when(jnp.logical_not(far))(lambda: launch(cm_sides[1:]))
    z_copy.wait_recv()
    w_copy.wait_recv()
    for k in range(1, R):
        tell(ready.at[1], k)
    z0_r = dot_nn(zrecv[...], hots[1])
    zz[1] = z0_r

    col = lax.broadcasted_iota(jnp.int32, (C, W), 1)
    cold = lax.broadcasted_iota(jnp.int32, (C, 128), 1)
    diag = cold == lax.broadcasted_iota(jnp.int32, (C, 128), 0)

    def pick(value, lane):
        return jnp.sum(jnp.where(col == lane, value, 0.0), axis=1, keepdims=True)

    fold = C == 16 and W == 128 and NC < 64

    def packed(value):
        return value[:8] + pltpu.roll(value[8:], 64, 1) if fold else value

    def unpacked(value):
        if not fold:
            return value
        low = lax.broadcasted_iota(jnp.int32, value.shape, 1) < 64
        return jnp.concatenate(
            [jnp.where(low, value, 0.0), pltpu.roll(jnp.where(low, 0.0, value), 64, 1)], axis=0
        )

    def spread(step, store, ssem, rsem):
        count = store.shape[1]
        slot = me if count == G else s

        def one(k):
            who = peer(k)[1] if count == G else {"sub": lax.rem(s + k + 1, S)}
            remote(store.at[step, slot], store.at[step, slot], ssem.at[step], rsem.at[step], who).start()

        each(count - 1, one)

    def gathered_sum(step, store, ssem, rsem, zero):
        count = store.shape[1]
        rest = store.at[step, pl.ds(0, count - 1)]
        remote(rest, rest, ssem.at[step], rsem.at[step], {"sub": nxt}).wait_recv()
        if count <= 8:
            total = store[step, 0]
            for g in range(1, count):
                total = total + store[step, g]
            return total
        return lax.fori_loop(0, count, lambda g, t: t + store[step, g], zero)

    def split(d, z):
        for j in range(half_r):
            zs[d * half_r + j] = z[:, j * B : (j + 1) * B]

    def product(step, local, r_left, z_left):
        blocks[step, r] = local.astype(BF)
        mine = blocks.at[step, r]
        delta = jnp.sum(zs[r] * local, axis=1, keepdims=True)
        dk[step, me] = jnp.sum(jnp.where(diag, delta, 0.0), axis=0, keepdims=True)
        if step == 0:
            corner = led[...]
        else:
            gamma = jnp.sum(r_left * z_left, axis=1, keepdims=True)
            corner = jnp.where(col == NC, gamma, 0.0)
        for q in range(half_r if step == 0 else 0, R):
            corner = corner + dot_nt(zs[q].astype(BF), mm[q, 0:W])
        pk[step, s] = packed(corner)
        nbr = blocks.at[step, pl.ds(R, R)]
        sides = [to_side(mine, nbr, blk_ssem.at[step], nbr_rsem.at[step, k], k) for k in range(R)]
        rows = [to_row(mine, blocks.at[step], blk_ssem.at[step], own_rsem.at[step, k - 1], k) for k in range(1, R)]

        def slopes(last):
            for ds in range(S):
                for dr in range(R):
                    distant = 1 < ds < S - 1 and dr > 0
                    if ds + dr > 0 and distant == last:
                        who = {"sub": lax.rem(s + ds, S), "row": lax.rem(r + dr, R)}
                        remote(dk.at[0, me], dk.at[0, me], dk_ssem.at[0], dk_rsem.at[0], who).start()

        if step == 0:
            spread(step, pk, pk_ssem, pk_rsem)
            launch(rows)
            slopes(False)
            launch(sides[1:] + sides[:1])
            pl.semaphore_wait(ready.at[1], R - 1)
            slopes(True)
        else:
            spread(step, pk, pk_ssem, pk_rsem)
            pl.when(side == 0)(lambda: launch(rows))
            spread(step, dk, dk_ssem, dk_rsem)
            pl.when(side == 1)(lambda: launch(sides[1:] + sides[:1]))

    def solve(step):
        total = unpacked(gathered_sum(step, pk, pk_ssem, pk_rsem, jnp.zeros(pk.shape[2:], F32)))
        t_hi = total.astype(BF)
        t_lo = (total - t_hi.astype(F32)).astype(BF)
        solved = dot_nn(jnp.concatenate([t_hi, t_lo, t_hi], axis=1), cinv_p[...].astype(BF))
        back = solved.astype(BF)
        gamma = pick(total, NC)
        bend = jnp.sum(total * back.astype(F32), axis=1, keepdims=True)
        return back, gamma, bend

    def bent(back, first, count):
        twice = jnp.concatenate([back, back], axis=1)
        return jnp.concatenate([dot_nn(twice, mm[first + j]) for j in range(count)], axis=1)

    def slope(step, total, bend):
        return jnp.sum(jnp.where(diag, total, 0.0), axis=1, keepdims=True) + bend

    def meet_own(step):
        for k in range(1, R):
            q = lax.rem(r + R - k, R)
            take = functools.partial(wait_slot, blocks.at[step], own_rsem.at[step, k - 1], q)
            if step == 0:
                take()
            else:
                pl.when(q < half_r)(take)

    def meet(step, d):
        for j in range(half_r):
            q = (1 - d) * half_r + j
            wait_slot(blocks.at[step], nbr_rsem.at[step, lax.rem(r - q + R, R)], R + q)

    def meeting(step, d):
        start = (1 - d) * half_r
        theirs = jnp.concatenate([blocks[step, R + start + j] for j in range(half_r)], axis=1)
        mine = jnp.concatenate([blocks[step, d * half_r + j] for j in range(half_r)], axis=1)
        return mine.astype(F32) + dot_nn(theirs, hots[d])

    split(0, z0)
    split(1, z0_r)
    local0 = acc[...] + dot_nn(z0_r.astype(BF), turned[1])
    product(0, local0, r0, z0)

    w_in = wrecv[...]
    w_hi = w_in.astype(BF)
    w_lo = (w_in - w_hi.astype(F32)).astype(BF)
    pad = lax.broadcasted_iota(jnp.int32, (16, H), 0)
    w_rows = jnp.where(pad == 0, w_hi.astype(F32), jnp.where(pad == 1, w_lo.astype(F32), 0.0))
    w_turned = dot_nn(w_rows.astype(BF), hots[1])
    wt[1] = w_turned[0:1] + w_turned[1:2]
    hot_next = hot_ids(nxt)
    hot_prev = hot_ids(prv)
    for k in range(R):
        wait_slot(cmn, cmn_rsem.at[k], lax.rem(r + R - k, R))
    for q in range(R):
        mm[q, W : 2 * W] = spreadout(hot_next if q < half_r else hot_prev, cmn[q]).astype(BF)
    right = dot_nn(jnp.concatenate([mm[q, W : 2 * W] for q in range(half_r)], axis=1), hots[1]).astype(BF)
    left = dot_nn(jnp.concatenate([mm[q, W : 2 * W] for q in range(half_r, R)], axis=1), hots[0]).astype(BF)
    for q in range(R):
        at = (q % half_r) * B
        mm[q, W : 2 * W] = (left if q < half_r else right)[:, at : at + B]

    early = jnp.where(s == 0, 1, 0)
    late = 1 - early
    meet_own(0)
    meet(0, early)
    met[early] = meeting(0, early)
    back0, gamma0, bend0 = solve(0)
    fixed[early] = bent(back0, early * half_r, half_r)
    steep0 = gathered_sum(0, dk, dk_ssem, dk_rsem, jnp.zeros((1, 128), F32))
    delta0 = slope(0, steep0, bend0)
    alpha0 = gamma0 / delta0

    fixed[late] = bent(back0, late * half_r, half_r)

    def advance(d):
        met[d] = (met[d] + fixed[d]) * live[d]
        z = zz[d] - alpha0 * (wt[d] * met[d])
        split(d, z)
        return z.astype(BF)

    acc[...] = dot_nn(advance(early), turned[early])
    meet(0, late)
    met[late] = meeting(0, late)
    last = advance(late)
    wl0 = met[0]
    r1 = r0 - alpha0 * wl0
    z1 = jnp.concatenate([zs[q] for q in range(half_r)], axis=1)
    local1 = acc[...] + dot_nn(last, turned[late])
    product(1, local1, r1, z1)
    back1, gamma1, bend1 = solve(1)
    fix = bent(back1, 0, half_r)
    beta = gamma1 / gamma0
    steep1 = gathered_sum(1, dk, dk_ssem, dk_rsem, jnp.zeros((1, 128), F32))
    delta1 = slope(1, steep1, bend1)
    alpha1 = gamma1 / (delta1 - beta * gamma1 / alpha0)
    sol[...] = alpha0 * z0 + alpha1 * (z1 + beta * z0)
    part = r1 - (alpha1 * beta) * wl0
    meet_own(1)
    meet(1, 0)
    res[...] = part - alpha1 * ((meeting(1, 0) + fix) * live[0])

    z_copy.wait_send()
    w_copy.wait_send()
    for copy in cm_sides + cm_rows:
        copy.wait_send()
    for step in range(2):
        def sent(count):
            gone = blocks.at[step, pl.ds(0, count)]
            remote(gone, gone, blk_ssem.at[step], blk_ssem.at[step], {"sub": nxt}).wait_send()

        if step == 0:
            sent(2 * R - 1)
        else:
            pl.when(side == 0)(functools.partial(sent, R - 1))
            pl.when(side == 1)(functools.partial(sent, R))
        for store, ssem, rsem in ((pk, pk_ssem, pk_rsem), (dk, dk_ssem, dk_rsem)):
            rest = store.at[step, pl.ds(0, store.shape[1] - 1)]
            remote(rest, rest, ssem.at[step], rsem.at[step], {"sub": nxt}).wait_send()


def finish(a, b, x, y, sem):
    first = pltpu.make_async_copy(a, x.at[0], sem.at[0])
    second = pltpu.make_async_copy(b, y.at[0], sem.at[1])
    first.start()
    second.start()
    first.wait()
    second.wait()


def per_device(S, R, loads, weights, dual_ops, corner_maps, coarse_inverse, corner_ids,
               iface_sizes, left_partner, right_partner):
    _, C, H = loads.shape
    _, B, full = dual_ops.shape
    J = corner_maps.shape[1]
    NC = coarse_inverse.shape[0]
    W = (NC + 1 + 127) // 128 * 128
    G = S * R
    fold = (16 * (J // 16), B + B // 2) if J % 16 == 8 and J < 32 else (J, B)
    DMA = pltpu.SemaphoreType.DMA
    hbm = pl.BlockSpec(memory_space=pltpu.HBM)
    vmem = pl.BlockSpec(memory_space=pltpu.VMEM)
    given = [
        pltpu.with_memory_space_constraint(x, pltpu.HBM)
        for x in (loads, weights, dual_ops, corner_maps, coarse_inverse, corner_ids, iface_sizes,
                  left_partner, right_partner)
    ]
    held = pltpu.VMEM((C, H), F32)
    made = pl.pallas_call(
        functools.partial(kernel, S, R),
        out_shape=(held, held),
        in_specs=[hbm] * 9,
        out_specs=(vmem, vmem),
        scratch_shapes=[
            pltpu.VMEM((C, H), F32), pltpu.VMEM((1, H), F32), pltpu.VMEM((B, full), BF),
            pltpu.VMEM((NC, NC), F32), pltpu.VMEM((3 * W, W), F32), pltpu.VMEM(corner_ids.shape, jnp.int32),
            pltpu.VMEM((1, H), jnp.int32), pltpu.VMEM((1, H), jnp.int32), pltpu.SMEM(iface_sizes.shape, jnp.int32),
            pltpu.VMEM((C, H), BF), pltpu.VMEM((C, H), BF), pltpu.VMEM((1, H), F32),
            pltpu.VMEM((J, B), BF), pltpu.VMEM((R,) + fold, BF), pltpu.VMEM((R,) + fold, BF),
            pltpu.VMEM((R, 2 * W, B), BF),
            pltpu.VMEM((2, H, H), BF), pltpu.VMEM((R, C, B), F32), pltpu.VMEM((C, B), F32),
            pltpu.VMEM((2, H, B), BF), pltpu.VMEM((2, C, H), F32), pltpu.VMEM((2, 1, H), F32), pltpu.VMEM((2, 1, H), F32),
            pltpu.VMEM((2, C, H), F32), pltpu.VMEM((2, C, H), F32),
            pltpu.VMEM((2, 2 * R, C, B), BF), pltpu.VMEM((2, S, 8 if C == 16 and W == 128 and NC < 64 else C, W), F32),
            pltpu.VMEM((2, G, 1, 128), F32),
            DMA((8,)), DMA, DMA((4,)), DMA((R - 1,)), DMA((R - 1,)), DMA((R,)), DMA((R,)),
            DMA((2,)), DMA((2, R - 1)), DMA((2, R)), DMA((2,)), DMA((2,)), DMA((2,)), DMA((2,)), pltpu.SemaphoreType.REGULAR((2,)), pltpu.VMEM((C, W), F32),
        ],
        compiler_params=pltpu.CompilerParams(
            collective_id=0, has_side_effects=True, vmem_limit_bytes=LIMIT
        ),
    )(*given)
    done = jax.ShapeDtypeStruct((1, C, H), F32)
    return pl.pallas_call(
        finish,
        out_shape=(done, done),
        in_specs=[vmem] * 2,
        out_specs=(hbm, hbm),
        scratch_shapes=[DMA((2,))],
        compiler_params=pltpu.CompilerParams(vmem_limit_bytes=2**20),
    )(*[pltpu.with_memory_space_constraint(x, pltpu.VMEM) for x in made])


def solution(mesh):
    placed = (
        P(("parts", "sub"), "col", None),
        P(("parts", "sub"), None),
        P(("parts", "sub"), "row", None),
        P(("parts", "sub"), None, "row"),
        P("parts", None),
        P("parts", None),
        P("parts"),
        P(("parts", "sub"), None),
        P(("parts", "sub"), None),
    )
    return jax.shard_map(
        functools.partial(per_device, mesh.shape["sub"], mesh.shape["row"]),
        mesh=mesh,
        in_specs=placed,
        out_specs=(P(("parts", "sub"), "col", None), P(("parts", "sub"), "col", None)),
        check_vma=False,
    )
```
